32 devices in a mesh: dp: 4 (over y, x), fsdp: 8 (over z, core).
Axes of the slice: x: 2, y: 2, z: 4, core: 2. Of those that a mesh axis runs over, the one named last changes fastest.
Arguments:
- hidden: bfloat16 [16384, 4096], P(('dp', 'fsdp')), may hold values from -6 to 6
- queries: bfloat16 [16384, 2048], P(('dp', 'fsdp')), may hold values from -60 to 60
- cotangent: bfloat16 [16384, 2048], P(('dp', 'fsdp')), may hold values from -0.125 to 0.125
- point_start: bfloat16 [4096, 1024], P('fsdp', 'dp'), may hold values from -0.09375 to 0.09375
- point_mid: bfloat16 [4096, 1024], P('fsdp', 'dp'), may hold values from -0.09375 to 0.09375
- point_end: bfloat16 [4096, 1024], P('fsdp', 'dp'), may hold values from -0.09375 to 0.09375
- curve_time: float32 [1], replicated, may hold values from 0.15 to 0.85
Outputs:
- context: bfloat16 [16384, 2048], P(('dp', 'fsdp'))
- gradient: float32 [4096, 1024], P('fsdp', 'dp')
The draws below stay inside these ranges and needn't reach their ends.
All inputs are finite; a program needn't handle non-finite values.
Results may differ from the reference program's by a relative error of at most 0.0071.
Values may be sent and summed in bfloat16 or wider, within the bound.
A program may use at most 128 MiB of HBM per device.

```python
import math
import jax
import jax.numpy as jnp
from jax import lax

D = 4096
HQ = 16
KVH = 4
HD = 128
SEQ = 512
KVW = 512
TOKENS = 16384


def draw_queries(key, part):
    first_key = jax.random.fold_in(key, 0)
    base_draw = jnp.clip(jax.random.normal(first_key, (TOKENS, HQ * HD), jnp.float32), -4.0, 4.0)
    return base_draw.astype(jnp.bfloat16)


def spiked(drawn, own_key, source, target, blocks, factor):
    owner, partner = [(jnp.arange(drawn.shape[position]) // (drawn.shape[position] // blocks)).reshape([-1 if axis == position else 1 for axis in range(drawn.ndim)]) for position in (source, target)]
    chosen = jax.random.permutation(own_key, blocks)[partner]
    strong = (owner == chosen) | (owner == (partner + blocks // 2) % blocks)
    return jnp.where(strong, factor * drawn, drawn)


def levels(stream_key, extent, cuts, least, top_value):
    gain = 1.0
    for axis_at, parts in cuts:
        steps = jax.random.uniform(jax.random.fold_in(jax.random.fold_in(stream_key, 6), axis_at), (parts,), jnp.float32, least / len(cuts), top_value / len(cuts))
        gain = gain * jnp.repeat(jnp.exp(steps), extent[axis_at] // parts).reshape((-1,) + (1,) * (len(extent) - 1 - axis_at))
    return gain


def centred(own_key, dims, scale, limit, cuts=(), held_as=jnp.bfloat16):
    entries = scale * jax.random.normal(own_key, dims, jnp.float32)
    if cuts:
        entries = entries * levels(own_key, dims, cuts, -0.22, 0.18)
    return jnp.clip(entries, -limit, limit).astype(held_as)


def heavy_noise(own_key, extent, scale, reach, cuts, heavy, held_as=jnp.bfloat16):
    values = scale * jax.random.normal(own_key, extent, jnp.float32)
    if cuts:
        values = values * levels(own_key, extent, cuts, -0.22, 0.18)
    return jnp.clip(spiked(values, jax.random.fold_in(own_key, 3), *heavy), -reach, reach).astype(held_as)


def setup_inputs(seed: int = 0) -> dict:
    splits = jax.random.split(jax.random.key(seed), 8)
    return {
        "hidden": heavy_noise(splits[0], (TOKENS, D), 1.0, 6.0, ((0, 32),), (0, 1, 32, 2.75)),
        "queries": draw_queries(jax.random.fold_in(splits[7], 71), 0),
        "cotangent": centred(splits[2], (TOKENS, HQ * HD), (TOKENS ** -0.5), 0.125, ((0, 32),)),
        "point_start": centred(splits[3], (D, 2 * KVW), D ** -0.5, 0.09375, ((0, 8), (1, 4))),
        "point_mid": centred(splits[4], (D, 2 * KVW), D ** -0.5, 0.09375, ((0, 8), (1, 4))),
        "point_end": centred(splits[5], (D, 2 * KVW), D ** -0.5, 0.09375, ((0, 8), (1, 4))),
        "curve_time": jnp.clip(jax.random.uniform(splits[6], (1,), jnp.float32, 0.15, 0.85), 0.15, 0.85),
    }


def rope_tables(seq_len, head_dim):
    positions = jnp.arange(seq_len, dtype=jnp.float32)[:, None]
    halves_index = jnp.arange(head_dim // 2, dtype=jnp.float32)[None, :]
    inverse = jnp.exp(-(2.0 * halves_index / head_dim) * math.log(500000.0))
    angles = positions * inverse
    cosine = jnp.concatenate([jnp.cos(angles), jnp.cos(angles)], axis=1)
    sine_t = jnp.concatenate([jnp.sin(angles), jnp.sin(angles)], axis=1)
    return (cosine, sine_t)

def rotate(values_in):
    half_size = values_in.shape[-1] // 2
    return jnp.concatenate([-values_in[..., half_size:], values_in[..., :half_size]], axis=-1)

def rotate_back(values_in):
    half_size = values_in.shape[-1] // 2
    return jnp.concatenate([values_in[..., half_size:], -values_in[..., :half_size]], axis=-1)

def attend(kv_rows, query_rows, grad_rows, kv_heads, head_dim):
    seq_len = kv_rows.shape[0]
    kv_width = kv_heads * head_dim
    group_size = query_rows.shape[1] // kv_width
    width_head = group_size * head_dim
    cosine, sine_t = rope_tables(seq_len, head_dim)
    causal = jnp.arange(seq_len)[:, None] >= jnp.arange(seq_len)[None, :]
    score_scale = 1.0 / math.sqrt(head_dim)
    contexts = []
    key_grads = []
    value_grads = []
    for kv_head in range(kv_heads):
        keys_raw = kv_rows[:, kv_head * head_dim:(kv_head + 1) * head_dim].astype(jnp.float32)
        values_head = kv_rows[:, kv_width + kv_head * head_dim:kv_width + (kv_head + 1) * head_dim].astype(jnp.float32)
        keys_head = (keys_raw * cosine + rotate(keys_raw) * sine_t).astype(jnp.bfloat16).astype(jnp.float32)
        query_head = query_rows[:, kv_head * width_head:(kv_head + 1) * width_head].reshape(seq_len, group_size, head_dim).astype(jnp.float32)
        grad_head = grad_rows[:, kv_head * width_head:(kv_head + 1) * width_head].reshape(seq_len, group_size, head_dim).astype(jnp.float32)
        scores = jnp.einsum('sgd,td->gst', query_head, keys_head) * score_scale
        scores = jnp.where(causal[None], scores, -1e+30)
        top_score = lax.optimization_barrier(jnp.max(scores, axis=-1, keepdims=True))
        weights_exp = jnp.exp(scores - top_score)
        probs = weights_exp / lax.optimization_barrier(jnp.sum(weights_exp, axis=-1, keepdims=True))
        probs_low = probs.astype(jnp.bfloat16).astype(jnp.float32)
        context_head = jnp.einsum('gst,td->sgd', probs_low, values_head).astype(jnp.bfloat16)
        contexts.append(context_head.reshape(seq_len, width_head))
        prob_grad = jnp.einsum('sgd,td->gst', grad_head, values_head)
        value_grads.append(jnp.einsum('gst,sgd->td', probs_low, grad_head))
        score_grad = probs * (prob_grad - lax.optimization_barrier(jnp.sum(prob_grad * probs, axis=-1, keepdims=True))) * score_scale
        score_low = score_grad.astype(jnp.bfloat16).astype(jnp.float32)
        rot_grad = jnp.einsum('gst,sgd->td', score_low, query_head)
        key_grads.append(rot_grad * cosine + rotate_back(rot_grad * sine_t))
    context_rows = jnp.concatenate(contexts, axis=1)
    kv_grad = jnp.concatenate(key_grads + value_grads, axis=1).astype(jnp.bfloat16)
    return (context_rows, kv_grad)

def reference(hidden, queries, cotangent, point_start, point_mid, point_end, curve_time):
    t_value = curve_time[0]
    blended = ((1.0 - t_value) ** 2 * point_start.astype(jnp.float32) + 2.0 * t_value * (1.0 - t_value) * point_mid.astype(jnp.float32) + t_value ** 2 * point_end.astype(jnp.float32)).astype(jnp.bfloat16)
    kv_rows = jnp.dot(hidden, blended, preferred_element_type=jnp.float32).astype(jnp.bfloat16)
    seq_count = hidden.shape[0] // SEQ

    def one_sequence(items):
        return attend(items[0], items[1], items[2], KVH, HD)
    context_all, grad_all = lax.map(one_sequence, (kv_rows.reshape(seq_count, SEQ, -1), queries.reshape(seq_count, SEQ, -1), cotangent.reshape(seq_count, SEQ, -1)))
    context = context_all.reshape(hidden.shape[0], -1)
    kv_grad = grad_all.reshape(hidden.shape[0], -1)
    gradient = jnp.dot(hidden.T, kv_grad, preferred_element_type=jnp.float32) * (2.0 * t_value * (1.0 - t_value))
    return (context, gradient)
```

```python
import functools
import math

import jax
import jax.numpy as jnp
from jax import lax
from jax.experimental import pallas as pl
from jax.experimental.pallas import tpu as pltpu
from jax.sharding import PartitionSpec as P

HD = 128
BQ = 256
MESH = pl.DeviceIdType.MESH
VMEM_LIMIT = 60 * 1024 * 1024


def rope_tables(seq_len, head_dim):
    shape = (seq_len, head_dim)
    positions = lax.broadcasted_iota(jnp.int32, shape, 0).astype(jnp.float32)
    column = lax.broadcasted_iota(jnp.int32, shape, 1)
    halves_index = jnp.where(column < head_dim // 2, column, column - head_dim // 2).astype(jnp.float32)
    inverse = jnp.exp(-(2.0 * halves_index / head_dim) * math.log(500000.0))
    angles = positions * inverse
    cosine, sine_t = jnp.cos(angles), jnp.sin(angles)
    return (cosine, sine_t)


def rotate(x):
    half = x.shape[-1] // 2
    return jnp.concatenate([-x[..., half:], x[..., :half]], axis=-1)


def rotate_back(x):
    half = x.shape[-1] // 2
    return jnp.concatenate([x[..., half:], -x[..., :half]], axis=-1)


NN = (((1,), (0,)), ((), ()))
NT = (((1,), (1,)), ((), ()))
TN = (((0,), (0,)), ((), ()))


def mm(x, y, dims=NN):
    return lax.dot_general(x, y, dims, preferred_element_type=jnp.float32)


ORDER = ((1, 0), (0, 1))


def place(dims):
    dp, fs = lax.axis_index("dp"), lax.axis_index("fsdp")
    return (dp // dims[1], dp % dims[1], fs // 2), fs % 2


def target(dims, at, core, axis=None, offset=0):
    at = list(at)
    if axis is not None:
        at[axis] = (at[axis] + offset + dims[axis]) % dims[axis]
    return (at[0] * dims[1] + at[1], at[2] * 2 + core)


def send(src, dst, send_sem, recv_sem, peer):
    return pltpu.make_async_remote_copy(
        src_ref=src, dst_ref=dst, send_sem=send_sem, recv_sem=recv_sem,
        device_id=peer, device_id_type=MESH)


def all_peers(dims, at, core):
    peers = [target(dims, at, core, axis, k) for axis in range(3) for k in range(1, dims[axis])]
    return peers + [target(dims, at, 1 - core)]


def attend_head(keys_at, values_at, q_cols, kv, q_ref, g_ref, cos_ref, sin_ref, ctx_ref, y_ref, kg, vg):
    seq = kv.shape[0]
    group = q_cols[1] // HD
    scale = 1.0 / math.sqrt(HD)
    to_base2 = scale * math.log2(math.e)

    def cols(g):
        return pl.ds(pl.multiple_of(q_cols[0] + g * HD, HD), HD)

    raw = kv[:, keys_at].astype(jnp.float32)
    cosine, sine_t = cos_ref[...], sin_ref[...]
    keys = (raw * cosine + rotate(raw) * sine_t).astype(jnp.bfloat16)
    values = kv[:, values_at]
    values_t = values.astype(jnp.float32).T.astype(jnp.bfloat16)
    kg[...] = jnp.zeros_like(kg)
    vg[...] = jnp.zeros_like(vg)
    for start in range(0, seq, BQ):
        nk = start + BQ
        rows = slice(start, nk)
        qs = jnp.concatenate([q_ref[rows, cols(g)] for g in range(group)], axis=0)
        gs = jnp.concatenate([g_ref[rows, cols(g)] for g in range(group)], axis=0)
        s = mm(keys[:nk], qs, NT)
        key_at = lax.broadcasted_iota(jnp.int32, (BQ, group * BQ), 0)
        query_at = lax.broadcasted_iota(jnp.int32, (BQ, group * BQ), 1) % BQ
        last = jnp.where(key_at <= query_at, s[start:], -1e30)
        s = last if start == 0 else jnp.concatenate([s[:start], last], axis=0)
        top = jnp.max(s, axis=0, keepdims=True)
        w = jnp.exp2((s - top) * to_base2)
        p = w * (1.0 / jnp.sum(w, axis=0, keepdims=True))
        p_low = p.astype(jnp.bfloat16)
        ctx_t = mm(values_t[:, :nk], p_low)
        dp = mm(values[:nk], gs, NT)
        vg[:nk] += mm(p_low, gs)
        delta = jnp.sum(dp * p, axis=0, keepdims=True)
        ds = (p * ((dp - delta) * scale)).astype(jnp.bfloat16)
        kg[:nk] += mm(ds, qs)
        ctx = ctx_t.T.astype(jnp.bfloat16)
        for g in range(group):
            ctx_ref[rows, cols(g)] = ctx[g * BQ:(g + 1) * BQ]
    rot = kg[...]
    y_ref[:, keys_at] = (rot * cosine + rotate_back(rot * sine_t)).astype(jnp.bfloat16)
    y_ref[:, values_at] = vg[...].astype(jnp.bfloat16)


def step_kernel(dims, t_ref, start_ref, mid_ref, end_ref, hidden_ref, query_ref, cot_ref, out_ctx, out_ref,
                pts, hid, x2, qv, gv, ctx, cos_ref, sin_ref, full, acc, kv, kg, vg, y1, y2, early,
                load_sem, x_send, x_recv, recv, z_send, c_send, y_send, y_recv, *more):
    s2, s3 = more[:2], more[2:4]
    halves = [more[4:15], more[15:26]]
    at, core = place(dims)
    depth = dims[2]
    across = dims[0] * dims[1]
    rows = start_ref.shape[0]
    half = rows // 2
    groups = full.shape[0]
    heads = across // 2
    other = target(dims, at, 1 - core)
    here = at[:2]


    def piece(p, c, h, zz, pos):
        col = pl.multiple_of((pos[0] * dims[1] + pos[1]) * HD, HD)
        return full.at[p, c, zz, pl.ds(h * half, half), pl.ds(col, HD)]

    def moved(axis, k):
        pos = [at[0], at[1]]
        pos[axis] = (pos[axis] + k) % dims[axis]
        return pos

    def push(p, h, zz, pos, send_sem, peer):
        ref = piece(p, core, h, zz, pos)
        return send(ref, ref, send_sem, recv.at[p, core, h, zz, pos[0], pos[1]], peer)

    def to_z(p, h, zz, side):
        return push(p, h, zz, here, z_send.at[p, h, side, zz], target(dims, at, core, 2, 1 - 2 * side))

    def onward(side):
        return ((side == 0) & (at[2] < depth - 1)) | ((side == 1) & (at[2] > 0))

    def near(k, act):
        @pl.loop(0, 2)
        def _(side):
            zz = at[2] + (2 * side - 1) * k
            pl.when((zz >= 0) & (zz < depth))(lambda: act(zz, side))

    def to_second(p, h, zz, k):
        d2 = ORDER[1 - h][0]
        return push(p, h, zz, here, s2[h].at[p, k - 1, zz], target(dims, at, core, d2, k))

    def to_third(p, h, zz, pos, k):
        d2, d3 = ORDER[1 - h]
        return push(p, h, zz, pos, s3[h].at[p, k - 1, zz, pos[d2]], target(dims, at, core, d3, k))

    def to_core(p, h, zz, pos):
        ref = piece(p, core, h, zz, pos)
        return send(ref, ref, c_send.at[p, h, zz, pos[0], pos[1]],
                    recv.at[p, core, h, zz, pos[0], pos[1]], other)

    def swap_x(zz):
        src = pl.multiple_of((2 * zz + 1 - core) * rows, rows)
        dst = pl.multiple_of(zz * rows, rows)
        return send(hidden_ref.at[:, pl.ds(src, rows)], x2.at[:, pl.ds(dst, rows)],
                    x_send.at[zz], x_recv.at[zz], other)

    def arrived(p, c, h, zz, pos):
        ref = piece(p, c, h, zz, pos)
        send(ref, ref, c_send.at[p, h, zz, pos[0], pos[1]], recv.at[p, c, h, zz, pos[0], pos[1]],
             other).wait_recv()

    def send_second(p, h, zz):
        for k in range(1, dims[ORDER[1 - h][0]]):
            to_second(p, h, zz, k).start()

    def send_own(p, h, zz):
        for k in range(1, dims[ORDER[1 - h][1]]):
            to_third(p, h, zz, here, k).start()
        to_core(p, h, zz, here).start()

    def start_z(p, zz, side):
        for h in range(2):
            to_z(p, h, zz, side).start()

    def own_z(p):
        @pl.loop(0, 2)
        def _(side):
            pl.when(onward(side))(lambda: start_z(p, at[2], side))

    def take_z(p, zz, side):
        for h in range(2):
            arrived(p, core, h, zz, here)
            pl.when(onward(side))(lambda: to_z(p, h, zz, side).start())
            if p == 0:
                send_second(p, h, zz)
                send_own(p, h, zz)

    def relay_second(p, zz):
        for h in range(2):
            d2, d3 = ORDER[1 - h]
            for k2 in range(1, dims[d2]):
                pos = moved(d2, k2)
                arrived(p, core, h, zz, pos)
                for k in range(1, dims[d3]):
                    to_third(p, h, zz, pos, k).start()
                to_core(p, h, zz, pos).start()

    def product(p, c, zz, first=False):
        x = hid[:, pl.ds(pl.multiple_of((2 * zz + c) * rows, rows), rows)]
        got = mm(x, full[p, c, zz])
        if first:
            acc[...] = got
        else:
            acc[...] += got

    def third(p, zz, first=False):
        for h in range(2):
            d2, d3 = ORDER[1 - h]
            for k3 in range(1, dims[d3]):
                for k2 in range(dims[d2]):
                    pos = moved(d3, k3)
                    pos[d2] = (at[d2] + k2) % dims[d2]
                    arrived(p, core, h, zz, pos)
                    to_core(p, h, zz, pos).start()
        product(p, core, zz, first)

    def from_core(p, zz):
        for h in range(2):
            for i in range(dims[0]):
                for j in range(dims[1]):
                    arrived(p, 1 - core, h, zz, (i, j))
        product(p, 1 - core, zz)

    def drain_gather():
        for p in range(groups):
            @pl.loop(0, depth)
            def _(zz):
                for h in range(2):
                    pl.when((zz <= at[2]) & (at[2] < depth - 1))(lambda: to_z(p, h, zz, 0).wait_send())
                    pl.when((zz >= at[2]) & (at[2] > 0))(lambda: to_z(p, h, zz, 1).wait_send())
                    d2, d3 = ORDER[1 - h]
                    for k in range(1, dims[d2]):
                        to_second(p, h, zz, k).wait_send()
                    for k in range(1, dims[d3]):
                        for k2 in range(dims[d2]):
                            to_third(p, h, zz, moved(d2, k2), k).wait_send()
                    for i in range(dims[0]):
                        for j in range(dims[1]):
                            to_core(p, h, zz, (i, j)).wait_send()


    def first_copy(p, h, k1, zz):
        d1 = ORDER[h][0]
        part, r1, s1, q1 = halves[h][0], halves[h][1], halves[h][5], halves[h][6]
        v1 = (at[d1] + k1) % dims[d1]
        return send(part.at[p, zz, v1], r1.at[p, k1 - 1, zz], s1.at[p, k1 - 1, zz], q1.at[p, k1 - 1, zz],
                    target(dims, at, core, d1, k1))

    def second_copy(p, h, k2, zz):
        d2 = ORDER[h][1]
        sum2, r2, t2, q2 = halves[h][2], halves[h][3], halves[h][7], halves[h][8]
        return send(sum2.at[p, k2 - 1, zz], r2.at[p, k2 - 1, zz], t2.at[p, k2 - 1, zz],
                    q2.at[p, k2 - 1, zz], target(dims, at, core, d2, k2))

    def third_copy(p, h, k):
        part, r3, t3, q3 = halves[h][0], halves[h][4], halves[h][9], halves[h][10]
        zz = (at[2] + k) % depth
        d1, d2 = ORDER[h]
        return send(part.at[p, zz, at[d1], at[d2]], r3.at[p, k - 1], t3.at[p, k - 1], q3.at[p, k - 1],
                    target(dims, at, core, 2, k))

    def swap_y(p):
        return send(y1.at[p], y2.at[p], y_send.at[p], y_recv.at[p], other)

    def partial_own(p):
        @pl.loop(0, depth)
        def _(zz):
            x = hid[:, pl.ds(pl.multiple_of((2 * zz + core) * rows, rows), rows)]
            early[zz] = mm(x, y1[p], TN)

    def partial_send(p):
        @pl.loop(1, depth + 1)
        def _(step):
            zz = (at[2] + step) % depth
            if p == 0:
                swap_x(zz).wait_recv()
            x = x2[:, pl.ds(pl.multiple_of(zz * rows, rows), rows)]
            r = (early[zz] + mm(x, y2[p], TN)).astype(jnp.bfloat16)
            for dp in range(across):
                where = (dp // dims[1], dp % dims[1])
                for h in range(2):
                    d1, d2 = ORDER[h]
                    halves[h][0][p, zz, where[d1], where[d2]] = (
                        r[h * half:(h + 1) * half, dp * HD:(dp + 1) * HD])
            for h in range(2):
                for k1 in range(1, dims[ORDER[h][0]]):
                    first_copy(p, h, k1, zz).start()

    def keep1(p, h, zz, v2):
        d1, d2 = ORDER[h]
        part, r1 = halves[h][0], halves[h][1]
        total = part[p, zz, at[d1], v2].astype(jnp.float32)
        for k1 in range(1, dims[d1]):
            total += r1[p, k1 - 1, zz, v2].astype(jnp.float32)
        return total

    def sum_second(p, step):
        zz = (at[2] + step) % depth
        for h in range(2):
            d1, d2 = ORDER[h]
            for k1 in range(1, dims[d1]):
                first_copy(p, h, k1, zz).wait_recv()
            for k2 in range(1, dims[d2]):
                v2 = (at[d2] + k2) % dims[d2]
                halves[h][2][p, k2 - 1, zz] = keep1(p, h, zz, v2).astype(jnp.bfloat16)
                second_copy(p, h, k2, zz).start()

    def keep2(p, h, zz):
        d1, d2 = ORDER[h]
        total = keep1(p, h, zz, at[d2])
        for k2 in range(1, dims[d2]):
            second_copy(p, h, k2, zz).wait_recv()
        for k2 in range(1, dims[d2]):
            total += halves[h][3][p, k2 - 1, zz].astype(jnp.float32)
        return total

    def sum_third(p, step):
        zz = (at[2] + step) % depth
        for h in range(2):
            d1, d2 = ORDER[h]
            halves[h][0][p, zz, at[d1], at[d2]] = keep2(p, h, zz).astype(jnp.bfloat16)
            third_copy(p, h, step).start()

    def finish(p):
        for h in range(2):
            total = keep2(p, h, at[2])
            for k in range(1, depth):
                third_copy(p, h, k).wait_recv()
                total += halves[h][4][p, k - 1].astype(jnp.float32)
            out_ref[h * half:(h + 1) * half, p * HD:(p + 1) * HD] = total

    def drain_reduce(p):
        @pl.loop(0, depth)
        def _(zz):
            for h in range(2):
                for k1 in range(1, dims[ORDER[h][0]]):
                    first_copy(p, h, k1, zz).wait_send()
                for k2 in range(1, dims[ORDER[h][1]]):
                    second_copy(p, h, k2, zz).wait_send()

        @pl.loop(1, depth)
        def _(k):
            for h in range(2):
                third_copy(p, h, k).wait_send()


    points = [pltpu.make_async_copy(ref, pts.at[i], load_sem.at[i])
              for i, ref in enumerate((start_ref, mid_ref, end_ref))]
    wholes = [pltpu.make_async_copy(ref, dst, load_sem.at[3 + i])
              for i, (ref, dst) in enumerate(((hidden_ref, hid), (query_ref, qv), (cot_ref, gv)))]
    for load in points + wholes:
        load.start()
    barrier = pltpu.get_barrier_semaphore()
    peers = all_peers(dims, at, core)
    for peer in peers:
        pl.semaphore_signal(barrier, inc=1, device_id=peer, device_id_type=MESH)
    for load in points:
        load.wait()
    t_value = t_ref[0]
    blended = (
        (1.0 - t_value) * (1.0 - t_value) * pts[0].astype(jnp.float32)
        + 2.0 * t_value * (1.0 - t_value) * pts[1].astype(jnp.float32)
        + t_value * t_value * pts[2].astype(jnp.float32)
    ).astype(jnp.bfloat16)
    col = pl.multiple_of((at[0] * dims[1] + at[1]) * HD, HD)
    for p in range(groups):
        full[p, core, at[2], :, pl.ds(col, HD)] = blended[:, p * HD:(p + 1) * HD]
    pl.semaphore_wait(barrier, len(peers))

    own_z(0)
    for h in range(2):
        send_second(0, h, at[2])
        send_own(0, h, at[2])

    @pl.loop(0, depth)
    def _(zz):
        swap_x(zz).start()

    cosine, sine_t = rope_tables(*cos_ref.shape)
    cos_ref[...] = cosine
    sin_ref[...] = sine_t

    near(1, lambda zz, side: take_z(0, zz, side))
    for p in range(1, groups):
        own_z(p)
    relay_second(0, at[2])
    wholes[0].wait()

    @pl.loop(2, depth)
    def _(k):
        near(k, lambda zz, side: take_z(0, zz, side))
        for p in range(1, groups):
            near(k - 1, lambda zz, side: take_z(p, zz, side))
        near(k - 1, lambda zz, side: relay_second(0, zz))
        pl.when(k == 2)(lambda: third(0, at[2], True))
        pl.when(k > 2)(lambda: near(k - 2, lambda zz, side: third(0, zz)))

    for p in range(1, groups):
        near(depth - 1, lambda zz, side: take_z(p, zz, side))
    near(depth - 1, lambda zz, side: relay_second(0, zz))

    def around(act):
        @pl.loop(0, depth)
        def _(i):
            act((at[2] + i) % depth)

    def send_group(p):
        around(lambda zz: [send_second(p, h, zz) for h in range(2)])
        around(lambda zz: [send_own(p, h, zz) for h in range(2)])

    if groups > 1:
        send_group(1)
    near(depth - 2, lambda zz, side: third(0, zz))
    from_core(0, at[2])

    @pl.loop(1, depth - 2)
    def _(k):
        near(k, lambda zz, side: from_core(0, zz))

    near(depth - 1, lambda zz, side: third(0, zz))
    near(depth - 2, lambda zz, side: from_core(0, zz))
    near(depth - 1, lambda zz, side: from_core(0, zz))
    wholes[1].wait()
    wholes[2].wait()

    share = depth // heads
    for p in range(groups):
        if p > 0:
            around(lambda zz: third(p, zz))
            around(lambda zz: from_core(p, zz))
        kv[...] = acc[...].astype(jnp.bfloat16)
        if p + 1 < groups:
            acc[...] = jnp.zeros_like(acc)

        @pl.loop(0, heads)
        def _(d):
            keys_at = pl.ds(pl.multiple_of(d * HD, HD), HD)
            values_at = pl.ds(pl.multiple_of((heads + d) * HD, HD), HD)
            width = qv.shape[1] // (heads * groups)
            attend_head(keys_at, values_at, ((d * groups + p) * width, width), kv, qv, gv, cos_ref,
                        sin_ref, ctx, y1.at[p], kg, vg)
            if p + 1 < groups:
                @pl.loop(0, share)
                def _(i):
                    relay_second(p + 1, (at[2] + d * share + i) % depth)
            if p > 0:
                @pl.when(d < heads - 1)
                def _():
                    @pl.loop(0, share)
                    def _(i):
                        sum_second(p - 1, d * share + i + 1)

        swap_y(p).start()
        if p == groups - 1:
            context = pltpu.make_async_copy(ctx, out_ctx, load_sem.at[6])
            context.start()
        if p + 2 < groups:
            send_group(p + 2)
        partial_own(p)
        if p > 0:
            @pl.loop((heads - 1) * share + 1, depth + 1)
            def _(step):
                sum_second(p - 1, step)
        swap_y(p).wait()
        partial_send(p)
        if p > 0:
            @pl.loop(1, depth)
            def _(step):
                sum_third(p - 1, step)

    drain_gather()
    last = groups - 1
    sum_second(last, 1)

    @pl.loop(2, depth + 1)
    def _(step):
        sum_second(last, step)
        sum_third(last, step - 1)

    for p in range(groups):
        finish(p)
    for p in range(groups):
        drain_reduce(p)

    @pl.loop(0, depth)
    def _(zz):
        swap_x(zz).wait_send()

    context.wait()


def run_step(dims, hidden, queries, cotangent, point_start, point_mid, point_end, curve_time):
    rows, cols = point_mid.shape
    seq = hidden.shape[0]
    a, b, z = dims
    groups = cols // HD
    half = rows // 2
    width = a * b * HD
    sem = pltpu.SemaphoreType.DMA

    def vm(*shape, dtype=jnp.bfloat16):
        return pltpu.VMEM(shape, dtype)

    f32 = jnp.float32
    scratch = [
        vm(3, rows, cols), vm(*hidden.shape), vm(seq, z * rows), vm(*queries.shape), vm(*cotangent.shape),
        vm(*queries.shape), vm(seq, HD, dtype=f32), vm(seq, HD, dtype=f32),
        vm(groups, 2, z, rows, width), vm(seq, width, dtype=f32), vm(seq, width),
        vm(seq, HD, dtype=f32), vm(seq, HD, dtype=f32),
        vm(groups, seq, width), vm(groups, seq, width), vm(z, rows, width, dtype=f32),
        sem((7,)), sem((z,)), sem((z,)), sem((groups, 2, 2, z, a, b)), sem((groups, 2, 2, z)),
        sem((groups, 2, z, a, b)), sem((groups,)), sem((groups,)),
    ]
    sizes = [[dims[axis] for axis in ORDER[1 - h]] for h in range(2)]
    scratch += [sem((groups, sizes[h][0] - 1, z)) for h in range(2)]
    scratch += [sem((groups, sizes[h][1] - 1, z, sizes[h][0])) for h in range(2)]
    for h in range(2):
        n1, n2 = dims[ORDER[h][0]], dims[ORDER[h][1]]
        scratch += [
            vm(groups, z, n1, n2, half, HD), vm(groups, n1 - 1, z, n2, half, HD),
            vm(groups, n2 - 1, z, half, HD), vm(groups, n2 - 1, z, half, HD),
            vm(groups, z - 1, half, HD),
            sem((groups, n1 - 1, z)), sem((groups, n1 - 1, z)),
            sem((groups, n2 - 1, z)), sem((groups, n2 - 1, z)),
            sem((groups, z - 1)), sem((groups, z - 1)),
        ]
    hbm = pl.BlockSpec(memory_space=pl.ANY)
    vmem = pl.BlockSpec(memory_space=pltpu.VMEM)
    return pl.pallas_call(
        functools.partial(step_kernel, dims),
        out_shape=(
            jax.ShapeDtypeStruct(queries.shape, jnp.bfloat16),
            jax.ShapeDtypeStruct((rows, cols), f32),
        ),
        in_specs=[pl.BlockSpec(memory_space=pltpu.SMEM)] + [hbm] * 6,
        out_specs=(hbm, vmem),
        scratch_shapes=scratch,
        compiler_params=pltpu.CompilerParams(
            collective_id=1, has_side_effects=True, vmem_limit_bytes=VMEM_LIMIT),
        name="bezier_step",
    )(curve_time, point_start, point_mid, point_end, hidden, queries, cotangent)


def local(dims, hidden, queries, cotangent, point_start, point_mid, point_end, curve_time):
    t_value = curve_time[0]
    context, gradient = run_step(dims, hidden, queries, cotangent, point_start, point_mid, point_end, curve_time)
    return (context, gradient * (2.0 * t_value * (1.0 - t_value)))


def solution(mesh):
    dp, fsdp = mesh.shape["dp"], mesh.shape["fsdp"]
    dims = (dp // 2, 2, fsdp // 2)
    return jax.shard_map(
        functools.partial(local, dims),
        mesh=mesh,
        in_specs=(
            P(("dp", "fsdp"), None),
            P(("dp", "fsdp"), None),
            P(("dp", "fsdp"), None),
            P("fsdp", "dp"),
            P("fsdp", "dp"),
            P("fsdp", "dp"),
            P(),
        ),
        out_specs=(P(("dp", "fsdp"), None), P("fsdp", "dp")),
        check_vma=False,
    )
```

```python
import functools
import math

import jax
import jax.numpy as jnp
from jax import lax
from jax.experimental import pallas as pl
from jax.experimental.pallas import tpu as pltpu
from jax.sharding import PartitionSpec as P

HD = 128
BQ = 256
MESH = pl.DeviceIdType.MESH
VMEM_LIMIT = 60 * 1024 * 1024


def rope_tables(seq_len, head_dim):
    shape = (seq_len, head_dim)
    positions = lax.broadcasted_iota(jnp.int32, shape, 0).astype(jnp.float32)
    column = lax.broadcasted_iota(jnp.int32, shape, 1)
    halves_index = jnp.where(column < head_dim // 2, column, column - head_dim // 2).astype(jnp.float32)
    inverse = jnp.exp(-(2.0 * halves_index / head_dim) * math.log(500000.0))
    angles = positions * inverse
    cosine, sine_t = jnp.cos(angles), jnp.sin(angles)
    return (cosine, sine_t)


def rotate(x):
    half = x.shape[-1] // 2
    return jnp.concatenate([-x[..., half:], x[..., :half]], axis=-1)


def rotate_back(x):
    half = x.shape[-1] // 2
    return jnp.concatenate([x[..., half:], -x[..., :half]], axis=-1)


NN = (((1,), (0,)), ((), ()))
NT = (((1,), (1,)), ((), ()))
TN = (((0,), (0,)), ((), ()))


def mm(x, y, dims=NN):
    return lax.dot_general(x, y, dims, preferred_element_type=jnp.float32)


ORDER = ((1, 0), (0, 1))


def place(dims):
    dp, fs = lax.axis_index("dp"), lax.axis_index("fsdp")
    return (dp // dims[1], dp % dims[1], fs // 2), fs % 2


def target(dims, at, core, axis=None, offset=0):
    at = list(at)
    if axis is not None:
        at[axis] = (at[axis] + offset + dims[axis]) % dims[axis]
    return (at[0] * dims[1] + at[1], at[2] * 2 + core)


def send(src, dst, send_sem, recv_sem, peer):
    return pltpu.make_async_remote_copy(
        src_ref=src, dst_ref=dst, send_sem=send_sem, recv_sem=recv_sem,
        device_id=peer, device_id_type=MESH)


def all_peers(dims, at, core):
    peers = [target(dims, at, core, axis, k) for axis in range(3) for k in range(1, dims[axis])]
    return peers + [target(dims, at, 1 - core)]


def attend_head(keys_at, values_at, q_cols, kv, q_ref, g_ref, cos_ref, sin_ref, ctx_ref, y_ref, kg, vg):
    seq = kv.shape[0]
    group = q_cols[1] // HD
    scale = 1.0 / math.sqrt(HD)
    to_base2 = scale * math.log2(math.e)

    def cols(g):
        return pl.ds(pl.multiple_of(q_cols[0] + g * HD, HD), HD)

    raw = kv[:, keys_at].astype(jnp.float32)
    cosine, sine_t = cos_ref[...], sin_ref[...]
    keys = (raw * cosine + rotate(raw) * sine_t).astype(jnp.bfloat16)
    values = kv[:, values_at]
    values_t = values.astype(jnp.float32).T.astype(jnp.bfloat16)
    kg[...] = jnp.zeros_like(kg)
    vg[...] = jnp.zeros_like(vg)
    for start in range(0, seq, BQ):
        nk = start + BQ
        rows = slice(start, nk)
        qs = jnp.concatenate([q_ref[rows, cols(g)] for g in range(group)], axis=0)
        gs = jnp.concatenate([g_ref[rows, cols(g)] for g in range(group)], axis=0)
        s = mm(keys[:nk], qs, NT)
        key_at = lax.broadcasted_iota(jnp.int32, (BQ, group * BQ), 0)
        query_at = lax.broadcasted_iota(jnp.int32, (BQ, group * BQ), 1) % BQ
        last = jnp.where(key_at <= query_at, s[start:], -1e30)
        s = last if start == 0 else jnp.concatenate([s[:start], last], axis=0)
        top = jnp.max(s, axis=0, keepdims=True)
        w = jnp.exp2((s - top) * to_base2)
        p = w * (1.0 / jnp.sum(w, axis=0, keepdims=True))
        p_low = p.astype(jnp.bfloat16)
        ctx_t = mm(values_t[:, :nk], p_low)
        dp = mm(values[:nk], gs, NT)
        vg[:nk] += mm(p_low, gs)
        delta = jnp.sum(dp * p, axis=0, keepdims=True)
        ds = (p * ((dp - delta) * scale)).astype(jnp.bfloat16)
        kg[:nk] += mm(ds, qs)
        ctx = ctx_t.T.astype(jnp.bfloat16)
        for g in range(group):
            ctx_ref[rows, cols(g)] = ctx[g * BQ:(g + 1) * BQ]
    rot = kg[...]
    y_ref[:, keys_at] = (rot * cosine + rotate_back(rot * sine_t)).astype(jnp.bfloat16)
    y_ref[:, values_at] = vg[...].astype(jnp.bfloat16)


def step_kernel(dims, t_ref, start_ref, mid_ref, end_ref, hidden_ref, query_ref, cot_ref, out_ctx, out_grad,
                pts, grad, hid, x2, qv, gv, ctx, cos_ref, sin_ref, full, acc, kv, kg, vg, y1, y2, early,
                load_sem, x_send, x_recv, y_send, y_recv, z_send, s_send, t_send, c_send,
                z_recv, t_recv, c_recv, *more):
    s_recv = more[:2]
    halves = [more[2:14], more[14:26]]
    at, core = place(dims)
    depth = dims[2]
    across = dims[0] * dims[1]
    rows = start_ref.shape[0]
    half = rows // 2
    groups = full.shape[0]
    last = groups - 1
    heads = across // 2
    other = target(dims, at, 1 - core)
    here = at[:2]

    def take_bytes(ref, sem):
        send(ref, ref, c_send.at[0], sem, other).wait_recv()

    def sent_bytes(ref, sem):
        send(ref, ref, sem, c_recv.at[0, 0], other).wait_send()


    def piece(p, c, h, zz, pos):
        col = pl.multiple_of((pos[0] * dims[1] + pos[1]) * HD, HD)
        return full.at[p, c, zz, pl.ds(h * half, half), pl.ds(col, HD)]

    def moved(axis, k):
        pos = [at[0], at[1]]
        pos[axis] = (pos[axis] + k) % dims[axis]
        return pos

    def push(p, h, zz, pos, send_sem, recv_sem, peer):
        ref = piece(p, core, h, zz, pos)
        return send(ref, ref, send_sem, recv_sem, peer)

    def near(k, act):
        @pl.loop(0, 2)
        def _(side):
            zz = at[2] + (2 * side - 1) * k
            pl.when((zz >= 0) & (zz < depth))(lambda: act(zz, side))

    def to_z(p, h, zz, side):
        push(p, h, zz, here, z_send.at[p, side, zz], z_recv.at[p, h, zz],
             target(dims, at, core, 2, 1 - 2 * side)).start()

    def onward(side):
        return ((side == 0) & (at[2] < depth - 1)) | ((side == 1) & (at[2] > 0))

    def to_second(p, h, zz, k):
        push(p, h, zz, here, s_send.at[p], s_recv[h].at[p, zz, k - 1],
             target(dims, at, core, ORDER[1 - h][0], k)).start()

    def to_third(p, h, zz, pos, k):
        push(p, h, zz, pos, t_send.at[p], t_recv.at[p, h, zz],
             target(dims, at, core, ORDER[1 - h][1], k)).start()

    def to_core(p, h, zz, pos):
        push(p, h, zz, pos, c_send.at[p], c_recv.at[p, zz], other).start()

    def swap_x(zz):
        src = pl.multiple_of((2 * zz + 1 - core) * rows, rows)
        dst = pl.multiple_of(zz * rows, rows)
        return send(hidden_ref.at[:, pl.ds(src, rows)], x2.at[:, pl.ds(dst, rows)],
                    x_send.at[0], x_recv.at[0], other)

    def own_z(p):
        @pl.loop(0, 2)
        def _(side):
            @pl.when(onward(side))
            def _():
                for h in range(2):
                    to_z(p, h, at[2], side)

    def send_all(p, h, zz):
        for k in range(1, dims[ORDER[1 - h][0]]):
            to_second(p, h, zz, k)
        for k in range(1, dims[ORDER[1 - h][1]]):
            to_third(p, h, zz, here, k)
        to_core(p, h, zz, here)

    def take_z(p, zz, side, more=True):
        for h in range(2):
            take_bytes(piece(p, core, h, zz, here), z_recv.at[p, h, zz])
            pl.when(onward(side))(lambda: to_z(p, h, zz, side))
            if more:
                send_all(p, h, zz)

    def relay_second(p, zz):
        for h in range(2):
            d2, d3 = ORDER[1 - h]
            for k2 in range(1, dims[d2]):
                pos = moved(d2, k2)
                take_bytes(piece(p, core, h, zz, pos), s_recv[h].at[p, zz, dims[d2] - k2 - 1])
                for k in range(1, dims[d3]):
                    to_third(p, h, zz, pos, k)
                to_core(p, h, zz, pos)

    def product(p, c, zz, first=False):
        x = hid[:, pl.ds(pl.multiple_of((2 * zz + c) * rows, rows), rows)]
        got = mm(x, full[p, c, zz])
        if first:
            acc[...] = got
        else:
            acc[...] += got

    def third(p, zz, first=False):
        for h in range(2):
            d2, d3 = ORDER[1 - h]
            count = (dims[d3] - 1) * dims[d2]
            take_bytes(full.at[p, core, zz, pl.ds(0, half), pl.ds(0, count * HD)], t_recv.at[p, h, zz])
            for k3 in range(1, dims[d3]):
                for k2 in range(dims[d2]):
                    pos = moved(d3, k3)
                    pos[d2] = (at[d2] + k2) % dims[d2]
                    to_core(p, h, zz, pos)
        product(p, core, zz, first)

    def from_core(p, zz):
        take_bytes(full.at[p, 1 - core, zz], c_recv.at[p, zz])
        product(p, 1 - core, zz)

    def drain_gather():
        seconds = dims[0] + dims[1] - 2
        thirds = (2 * across - dims[0] - dims[1]) // 2
        for p in range(groups):
            @pl.loop(0, depth)
            def _(zz):
                ref = full.at[p, core, zz, :, pl.ds(0, HD)]
                pl.when((zz <= at[2]) & (at[2] < depth - 1))(lambda: sent_bytes(ref, z_send.at[p, 0, zz]))
                pl.when((zz >= at[2]) & (at[2] > 0))(lambda: sent_bytes(ref, z_send.at[p, 1, zz]))

            sent_bytes(full.at[p, core, :, pl.ds(0, half), pl.ds(0, seconds * HD)], s_send.at[p])
            sent_bytes(full.at[p, core, :, :, pl.ds(0, thirds * HD)], t_send.at[p])
            sent_bytes(full.at[p, core], c_send.at[p])


    def first_copies(p, zz, same):
        for h in range(2):
            d1, d2 = ORDER[h]
            part, r1, q1 = halves[h][0], halves[h][1], halves[h][6 + same]
            for k1 in range(1, dims[d1]):
                v1 = (at[d1] + k1) % dims[d1]
                for k2 in (0,) if same else range(1, dims[d2]):
                    v2 = (at[d2] + k2) % dims[d2]
                    send(part.at[p, zz, v1, v2], r1.at[p, k1 - 1, zz, v2], halves[h][5].at[p], q1.at[p, zz],
                         target(dims, at, core, d1, k1)).start()

    def take_first(p, h, zz, same):
        count = 1 if same else dims[ORDER[h][1]] - 1
        take_bytes(halves[h][1].at[p, :, zz, pl.ds(0, count)], halves[h][6 + same].at[p, zz])

    def swap_y(p):
        return send(y1.at[p], y2.at[p], y_send.at[p], y_recv.at[p], other)

    def partial_own(p):
        @pl.loop(0, depth)
        def _(zz):
            x = hid[:, pl.ds(pl.multiple_of((2 * zz + core) * rows, rows), rows)]
            early[zz] = mm(x, y1[p], TN)

    def turn(step):
        return (at[2] + step) % depth

    def partial_sum(p, zz):
        x = x2[:, pl.ds(pl.multiple_of(zz * rows, rows), rows)]
        r = (early[zz] + mm(x, y2[p], TN)).astype(jnp.bfloat16)
        for dp in range(across):
            where = (dp // dims[1], dp % dims[1])
            for h in range(2):
                d1, d2 = ORDER[h]
                halves[h][0][p, zz, where[d1], where[d2]] = (
                    r[h * half:(h + 1) * half, dp * HD:(dp + 1) * HD])

    def keep1(p, h, zz, v2):
        d1, d2 = ORDER[h]
        part, r1 = halves[h][0], halves[h][1]
        total = part[p, zz, at[d1], v2].astype(jnp.float32)
        for k1 in range(1, dims[d1]):
            total += r1[p, k1 - 1, zz, v2].astype(jnp.float32)
        return total

    def sum_second(p, zz):
        for h in range(2):
            d2 = ORDER[h][1]
            sum2, r2 = halves[h][2], halves[h][3]
            take_first(p, h, zz, 0)
            for k2 in range(1, dims[d2]):
                v2 = (at[d2] + k2) % dims[d2]
                sum2[p, k2 - 1, zz] = keep1(p, h, zz, v2).astype(jnp.bfloat16)
                send(sum2.at[p, k2 - 1, zz], r2.at[p, k2 - 1, zz], halves[h][8].at[p], halves[h][9].at[p, zz],
                     target(dims, at, core, d2, k2)).start()

    def keep2(p, h, zz):
        d2 = ORDER[h][1]
        take_first(p, h, zz, 1)
        total = keep1(p, h, zz, at[d2])
        take_bytes(halves[h][3].at[p, :, zz], halves[h][9].at[p, zz])
        for k2 in range(1, dims[d2]):
            total += halves[h][3][p, k2 - 1, zz].astype(jnp.float32)
        return total

    def sum_third(p, step):
        zz = turn(step)
        for h in range(2):
            d1, d2 = ORDER[h]
            part, r3 = halves[h][0], halves[h][4]
            part[p, zz, at[d1], at[d2]] = keep2(p, h, zz).astype(jnp.bfloat16)
            send(part.at[p, zz, at[d1], at[d2]], r3.at[p, step - 1], halves[h][10].at[p], halves[h][11].at[p],
                 target(dims, at, core, 2, step)).start()

    def store(p):
        return pltpu.make_async_copy(grad.at[p], out_grad.at[:, pl.ds(p * HD, HD)], load_sem.at[7 + p])

    def finish(p):
        for h in range(2):
            total = keep2(p, h, at[2])
            take_bytes(halves[h][4].at[p], halves[h][11].at[p])
            for k in range(1, depth):
                total += halves[h][4][p, k - 1].astype(jnp.float32)
            grad[p, h * half:(h + 1) * half] = total
        store(p).start()

    def drain_reduce(p):
        for h in range(2):
            sent_bytes(halves[h][1].at[p], halves[h][5].at[p])
            sent_bytes(halves[h][3].at[p], halves[h][8].at[p])
            sent_bytes(halves[h][4].at[p], halves[h][10].at[p])


    points = [pltpu.make_async_copy(ref, pts.at[i], load_sem.at[i])
              for i, ref in enumerate((start_ref, mid_ref, end_ref))]
    wholes = [pltpu.make_async_copy(ref, dst, load_sem.at[3 + i])
              for i, (ref, dst) in enumerate(((hidden_ref, hid), (query_ref, qv), (cot_ref, gv)))]
    for load in points + wholes:
        load.start()
    barrier = pltpu.get_barrier_semaphore()
    peers = all_peers(dims, at, core)
    for peer in peers:
        pl.semaphore_signal(barrier, inc=1, device_id=peer, device_id_type=MESH)
    for load in points:
        load.wait()
    t_value = t_ref[0]
    blended = (
        (1.0 - t_value) * (1.0 - t_value) * pts[0].astype(jnp.float32)
        + 2.0 * t_value * (1.0 - t_value) * pts[1].astype(jnp.float32)
        + t_value * t_value * pts[2].astype(jnp.float32)
    ).astype(jnp.bfloat16)
    col = pl.multiple_of((at[0] * dims[1] + at[1]) * HD, HD)
    for p in range(groups):
        full[p, core, at[2], :, pl.ds(col, HD)] = blended[:, p * HD:(p + 1) * HD]
    pl.semaphore_wait(barrier, len(peers))

    def send_both(p, zz):
        for h in range(2):
            send_all(p, h, zz)

    own_z(0)
    for p in range(min(groups, 2)):
        send_both(p, at[2])

    @pl.loop(0, depth)
    def _(zz):
        swap_x(zz).start()

    cosine, sine_t = rope_tables(*cos_ref.shape)
    cos_ref[...] = cosine
    sin_ref[...] = sine_t

    def take_first_group(k):
        near(k, lambda zz, side: take_z(0, zz, side))

    def relay_first_group(k):
        near(k, lambda zz, side: relay_second(0, zz))

    take_first_group(1)
    relay_second(0, at[2])

    @pl.loop(2, depth)
    def _(k):
        take_first_group(k)
        if groups > 1:
            pl.when(k == depth - 2)(lambda: own_z(1))
        relay_first_group(k - 1)

    wholes[0].wait()
    if groups > 1:
        near(1, lambda zz, side: take_z(1, zz, side, False))
    third(0, at[2], True)
    relay_first_group(depth - 1)
    if groups > 1:
        near(1, lambda zz, side: send_both(1, zz))
    near(1, lambda zz, side: third(0, zz))
    from_core(0, at[2])

    @pl.loop(2, depth)
    def _(k):
        if groups > 1:
            pl.when(k < depth - 1)(lambda: near(k, lambda zz, side: take_z(1, zz, side)))
        near(k, lambda zz, side: third(0, zz))
        near(k - 1, lambda zz, side: from_core(0, zz))

    near(depth - 1, lambda zz, side: from_core(0, zz))
    if groups > 1:
        near(depth - 1, lambda zz, side: take_z(1, zz, side))
    wholes[1].wait()
    wholes[2].wait()

    def around(act):
        @pl.loop(0, depth)
        def _(i):
            act(turn(i))

    share = depth // heads
    early_steps = min(2, depth - 1)
    for p in range(groups):
        if p > 0:
            around(lambda zz: third(p, zz))
            around(lambda zz: from_core(p, zz))

            @pl.loop(1, early_steps + 1)
            def _(step):
                sum_second(p - 1, turn(step))

            @pl.loop(1, early_steps + 1)
            def _(step):
                first_copies(p - 1, turn(step), 1)
        kv[...] = acc[...].astype(jnp.bfloat16)
        if p < last:
            acc[...] = jnp.zeros_like(acc)

        @pl.loop(0, heads)
        def _(d):
            keys_at = pl.ds(pl.multiple_of(d * HD, HD), HD)
            values_at = pl.ds(pl.multiple_of((heads + d) * HD, HD), HD)
            width = qv.shape[1] // (heads * groups)
            attend_head(keys_at, values_at, ((d * groups + p) * width, width), kv, qv, gv, cos_ref,
                        sin_ref, ctx, y1.at[p], kg, vg)
            if p < last:
                @pl.loop(0, share)
                def _(i):
                    k = d * share + i
                    pl.when(k == 0)(lambda: relay_second(p + 1, at[2]))
                    pl.when(k > 0)(lambda: near(k, lambda zz, side: relay_second(p + 1, zz)))
            if p > 0:
                @pl.when(d == 0)
                def _():
                    @pl.loop(early_steps + 1, depth + 1)
                    def _(step):
                        sum_second(p - 1, turn(step))
                        first_copies(p - 1, turn(step), 1)

        swap_y(p).start()
        if p > 0:
            @pl.loop(1, early_steps + 1)
            def _(step):
                sum_third(p - 1, step)
        if p == last:
            context = pltpu.make_async_copy(ctx, out_ctx, load_sem.at[6])
            context.start()
        partial_own(p)
        if p == 0:
            take_bytes(x2, x_recv.at[0])
        swap_y(p).wait()
        if p < last:
            @pl.loop(1, depth + 1)
            def _(step):
                partial_sum(p, turn(step))
                first_copies(p, turn(step), 0)

    partial_sum(last, turn(1))
    first_copies(last, turn(1), 0)
    partial_sum(last, turn(2))
    first_copies(last, turn(2), 0)
    first_copies(last, turn(1), 1)

    @pl.loop(3, depth + 1)
    def _(step):
        partial_sum(last, turn(step))

    for p in range(last):
        @pl.loop(early_steps + 1, depth)
        def _(step):
            sum_third(p, step)

    sum_second(last, turn(1))
    first_copies(last, turn(2), 1)
    sum_second(last, turn(2))

    @pl.loop(3, depth)
    def _(step):
        first_copies(last, turn(step), 0)
        first_copies(last, turn(step), 1)

    first_copies(last, at[2], 0)
    for p in range(last):
        finish(p)
    drain_gather()
    sent_bytes(x2, x_send.at[0])

    @pl.loop(1, depth - 1)
    def _(step):
        sum_third(last, step)

    @pl.loop(3, depth)
    def _(step):
        sum_second(last, turn(step))

    first_copies(last, at[2], 1)
    sum_second(last, at[2])
    sum_third(last, depth - 1)
    for p in range(last):
        drain_reduce(p)
    finish(last)
    drain_reduce(last)
    context.wait()
    for p in range(groups):
        store(p).wait()


def run_step(dims, hidden, queries, cotangent, point_start, point_mid, point_end, curve_time):
    rows, cols = point_mid.shape
    seq = hidden.shape[0]
    a, b, z = dims
    groups = cols // HD
    half = rows // 2
    width = a * b * HD
    sem = pltpu.SemaphoreType.DMA

    def vm(*shape, dtype=jnp.bfloat16):
        return pltpu.VMEM(shape, dtype)

    f32 = jnp.float32
    scratch = [
        vm(3, rows, cols), vm(groups, rows, HD, dtype=f32), vm(*hidden.shape), vm(seq, z * rows),
        vm(*queries.shape), vm(*cotangent.shape),
        vm(*queries.shape), vm(seq, HD, dtype=f32), vm(seq, HD, dtype=f32),
        vm(groups, 2, z, rows, width), vm(seq, width, dtype=f32), vm(seq, width),
        vm(seq, HD, dtype=f32), vm(seq, HD, dtype=f32),
        vm(groups, seq, width), vm(groups, seq, width), vm(z, rows, width, dtype=f32),
        sem((7 + groups,)), sem((1,)), sem((1,)), sem((groups,)), sem((groups,)),
        sem((groups, 2, z)), sem((groups,)), sem((groups,)), sem((groups,)),
        sem((groups, 2, z)), sem((groups, 2, z)), sem((groups, z)),
    ]
    scratch += [sem((groups, z, dims[ORDER[1 - h][0]] - 1)) for h in range(2)]
    for h in range(2):
        n1, n2 = dims[ORDER[h][0]], dims[ORDER[h][1]]
        scratch += [
            vm(groups, z, n1, n2, half, HD), vm(groups, n1 - 1, z, n2, half, HD),
            vm(groups, n2 - 1, z, half, HD), vm(groups, n2 - 1, z, half, HD),
            vm(groups, z - 1, half, HD),
            sem((groups,)), sem((groups, z)), sem((groups, z)),
            sem((groups,)), sem((groups, z)),
            sem((groups,)), sem((groups,)),
        ]
    hbm = pl.BlockSpec(memory_space=pl.ANY)
    return pl.pallas_call(
        functools.partial(step_kernel, dims),
        out_shape=(
            jax.ShapeDtypeStruct(queries.shape, jnp.bfloat16),
            jax.ShapeDtypeStruct((rows, cols), f32),
        ),
        in_specs=[pl.BlockSpec(memory_space=pltpu.SMEM)] + [hbm] * 6,
        out_specs=(hbm, hbm),
        scratch_shapes=scratch,
        compiler_params=pltpu.CompilerParams(
            collective_id=1, has_side_effects=True, vmem_limit_bytes=VMEM_LIMIT),
        name="bezier_step",
    )(curve_time, point_start, point_mid, point_end, hidden, queries, cotangent)


def local(dims, hidden, queries, cotangent, point_start, point_mid, point_end, curve_time):
    t_value = curve_time[0]
    context, gradient = run_step(dims, hidden, queries, cotangent, point_start, point_mid, point_end, curve_time)
    return (context, gradient * (2.0 * t_value * (1.0 - t_value)))


def solution(mesh):
    dp, fsdp = mesh.shape["dp"], mesh.shape["fsdp"]
    dims = (dp // 2, 2, fsdp // 2)
    return jax.shard_map(
        functools.partial(local, dims),
        mesh=mesh,
        in_specs=(
            P(("dp", "fsdp"), None),
            P(("dp", "fsdp"), None),
            P(("dp", "fsdp"), None),
            P("fsdp", "dp"),
            P("fsdp", "dp"),
            P("fsdp", "dp"),
            P(),
        ),
        out_specs=(P(("dp", "fsdp"), None), P("fsdp", "dp")),
        check_vma=False,
    )
```

```python
import functools
import math

import jax
import jax.numpy as jnp
from jax import lax
from jax.experimental import pallas as pl
from jax.experimental.pallas import tpu as pltpu
from jax.sharding import PartitionSpec as P

HD = 128
BQ = 256
MESH = pl.DeviceIdType.MESH
VMEM_LIMIT = 60 * 1024 * 1024


def rope_tables(seq_len, head_dim):
    shape = (seq_len, head_dim)
    positions = lax.broadcasted_iota(jnp.int32, shape, 0).astype(jnp.float32)
    column = lax.broadcasted_iota(jnp.int32, shape, 1)
    halves_index = jnp.where(column < head_dim // 2, column, column - head_dim // 2).astype(jnp.float32)
    inverse = jnp.exp(-(2.0 * halves_index / head_dim) * math.log(500000.0))
    angles = positions * inverse
    cosine, sine_t = jnp.cos(angles), jnp.sin(angles)
    return (cosine, sine_t)


def rotate(x):
    half = x.shape[-1] // 2
    return jnp.concatenate([-x[..., half:], x[..., :half]], axis=-1)


def rotate_back(x):
    half = x.shape[-1] // 2
    return jnp.concatenate([x[..., half:], -x[..., :half]], axis=-1)


NN = (((1,), (0,)), ((), ()))
NT = (((1,), (1,)), ((), ()))
TN = (((0,), (0,)), ((), ()))


def mm(x, y, dims=NN):
    return lax.dot_general(x, y, dims, preferred_element_type=jnp.float32)


ORDER = ((1, 0), (0, 1))


def place(dims):
    dp, fs = lax.axis_index("dp"), lax.axis_index("fsdp")
    return (dp // dims[1], dp % dims[1], fs // 2), fs % 2


def target(dims, at, core, axis=None, offset=0):
    at = list(at)
    if axis is not None:
        at[axis] = (at[axis] + offset + dims[axis]) % dims[axis]
    return (at[0] * dims[1] + at[1], at[2] * 2 + core)


def send(src, dst, send_sem, recv_sem, peer):
    return pltpu.make_async_remote_copy(
        src_ref=src, dst_ref=dst, send_sem=send_sem, recv_sem=recv_sem,
        device_id=peer, device_id_type=MESH)


def all_peers(dims, at, core):
    peers = [target(dims, at, core, axis, k) for axis in range(3) for k in range(1, dims[axis])]
    return peers + [target(dims, at, 1 - core)]


def attend_head(keys_at, values_at, q_cols, kv, q_ref, g_ref, cos_ref, sin_ref, ctx_ref, y_ref, kg, vg):
    seq = kv.shape[0]
    group = q_cols[1] // HD
    scale = 1.0 / math.sqrt(HD)
    to_base2 = scale * math.log2(math.e)

    def cols(g):
        return pl.ds(pl.multiple_of(q_cols[0] + g * HD, HD), HD)

    raw = kv[:, keys_at].astype(jnp.float32)
    cosine, sine_t = cos_ref[...], sin_ref[...]
    keys = (raw * cosine + rotate(raw) * sine_t).astype(jnp.bfloat16)
    values = kv[:, values_at]
    values_t = values.astype(jnp.float32).T.astype(jnp.bfloat16)
    kg[...] = jnp.zeros_like(kg)
    vg[...] = jnp.zeros_like(vg)
    for start in range(0, seq, BQ):
        nk = start + BQ
        rows = slice(start, nk)
        qs = jnp.concatenate([q_ref[rows, cols(g)] for g in range(group)], axis=0)
        gs = jnp.concatenate([g_ref[rows, cols(g)] for g in range(group)], axis=0)
        s = mm(keys[:nk], qs, NT)
        key_at = lax.broadcasted_iota(jnp.int32, (BQ, group * BQ), 0)
        query_at = lax.broadcasted_iota(jnp.int32, (BQ, group * BQ), 1) % BQ
        last = jnp.where(key_at <= query_at, s[start:], -1e30)
        s = last if start == 0 else jnp.concatenate([s[:start], last], axis=0)
        top = jnp.max(s, axis=0, keepdims=True)
        w = jnp.exp2((s - top) * to_base2)
        p = w * (1.0 / jnp.sum(w, axis=0, keepdims=True))
        p_low = p.astype(jnp.bfloat16)
        ctx_t = mm(values_t[:, :nk], p_low)
        dp = mm(values[:nk], gs, NT)
        vg[:nk] += mm(p_low, gs)
        delta = jnp.sum(dp * p, axis=0, keepdims=True)
        ds = (p * ((dp - delta) * scale)).astype(jnp.bfloat16)
        kg[:nk] += mm(ds, qs)
        ctx = ctx_t.T.astype(jnp.bfloat16)
        for g in range(group):
            ctx_ref[rows, cols(g)] = ctx[g * BQ:(g + 1) * BQ]
    rot = kg[...]
    y_ref[:, keys_at] = (rot * cosine + rotate_back(rot * sine_t)).astype(jnp.bfloat16)
    y_ref[:, values_at] = vg[...].astype(jnp.bfloat16)


def step_kernel(dims, t_ref, start_ref, mid_ref, end_ref, hidden_ref, query_ref, cot_ref, ctx, grad,
                pts, hid, x2, qv, gv, cos_ref, sin_ref, full, acc, kv, kg, vg, y1, y2, early,
                load_sem, x_send, x_recv, y_send, y_recv, z_send, s_send, t_send, c_send,
                z_recv, t_recv, c_recv, *more):
    s_recv = more[:2]
    halves = [more[2:14], more[14:26]]
    at, core = place(dims)
    depth = dims[2]
    across = dims[0] * dims[1]
    rows = start_ref.shape[0]
    half = rows // 2
    groups = full.shape[0]
    last = groups - 1
    heads = across // 2
    other = target(dims, at, 1 - core)
    here = at[:2]

    def take_bytes(ref, sem):
        send(ref, ref, c_send.at[0], sem, other).wait_recv()

    def sent_bytes(ref, sem):
        send(ref, ref, sem, c_recv.at[0, 0], other).wait_send()


    def piece(p, c, h, zz, pos):
        col = pl.multiple_of((pos[0] * dims[1] + pos[1]) * HD, HD)
        return full.at[p, c, zz, pl.ds(h * half, half), pl.ds(col, HD)]

    def moved(axis, k):
        pos = [at[0], at[1]]
        pos[axis] = (pos[axis] + k) % dims[axis]
        return pos

    def push(p, h, zz, pos, send_sem, recv_sem, peer):
        ref = piece(p, core, h, zz, pos)
        return send(ref, ref, send_sem, recv_sem, peer)

    def near(k, act):
        @pl.loop(0, 2)
        def _(side):
            zz = at[2] + (2 * side - 1) * k
            pl.when((zz >= 0) & (zz < depth))(lambda: act(zz, side))

    def to_z(p, h, zz, side):
        push(p, h, zz, here, z_send.at[p, side, zz], z_recv.at[p, h, zz],
             target(dims, at, core, 2, 1 - 2 * side)).start()

    def onward(side):
        return ((side == 0) & (at[2] < depth - 1)) | ((side == 1) & (at[2] > 0))

    def to_second(p, h, zz, k):
        push(p, h, zz, here, s_send.at[p], s_recv[h].at[p, zz, k - 1],
             target(dims, at, core, ORDER[1 - h][0], k)).start()

    def to_third(p, h, zz, pos, k):
        push(p, h, zz, pos, t_send.at[p], t_recv.at[p, h, zz],
             target(dims, at, core, ORDER[1 - h][1], k)).start()

    def to_core(p, h, zz, pos):
        push(p, h, zz, pos, c_send.at[p], c_recv.at[p, zz], other).start()

    def swap_x(zz):
        src = pl.multiple_of((2 * zz + 1 - core) * rows, rows)
        dst = pl.multiple_of(zz * rows, rows)
        return send(hidden_ref.at[:, pl.ds(src, rows)], x2.at[:, pl.ds(dst, rows)],
                    x_send.at[0], x_recv.at[0], other)

    def own_z(p):
        @pl.loop(0, 2)
        def _(side):
            @pl.when(onward(side))
            def _():
                for h in range(2):
                    to_z(p, h, at[2], side)

    def send_all(p, h, zz):
        for k in range(1, dims[ORDER[1 - h][0]]):
            to_second(p, h, zz, k)
        for k in range(1, dims[ORDER[1 - h][1]]):
            to_third(p, h, zz, here, k)
        to_core(p, h, zz, here)

    def take_z(p, zz, side, more=True):
        for h in range(2):
            take_bytes(piece(p, core, h, zz, here), z_recv.at[p, h, zz])
            pl.when(onward(side))(lambda: to_z(p, h, zz, side))
            if more:
                send_all(p, h, zz)

    def relay_second(p, zz):
        for h in range(2):
            d2, d3 = ORDER[1 - h]
            for k2 in range(1, dims[d2]):
                pos = moved(d2, k2)
                take_bytes(piece(p, core, h, zz, pos), s_recv[h].at[p, zz, dims[d2] - k2 - 1])
                for k in range(1, dims[d3]):
                    to_third(p, h, zz, pos, k)
                to_core(p, h, zz, pos)

    def product(p, c, zz, first=False):
        x = hid[:, pl.ds(pl.multiple_of((2 * zz + c) * rows, rows), rows)]
        got = mm(x, full[p, c, zz])
        if first:
            acc[...] = got
        else:
            acc[...] += got

    def third(p, zz, first=False):
        for h in range(2):
            d2, d3 = ORDER[1 - h]
            count = (dims[d3] - 1) * dims[d2]
            take_bytes(full.at[p, core, zz, pl.ds(0, half), pl.ds(0, count * HD)], t_recv.at[p, h, zz])
            for k3 in range(1, dims[d3]):
                for k2 in range(dims[d2]):
                    pos = moved(d3, k3)
                    pos[d2] = (at[d2] + k2) % dims[d2]
                    to_core(p, h, zz, pos)
        product(p, core, zz, first)

    def from_core(p, zz):
        take_bytes(full.at[p, 1 - core, zz], c_recv.at[p, zz])
        product(p, 1 - core, zz)

    def drain_gather():
        seconds = dims[0] + dims[1] - 2
        thirds = (2 * across - dims[0] - dims[1]) // 2
        for p in range(groups):
            @pl.loop(0, depth)
            def _(zz):
                ref = full.at[p, core, zz, :, pl.ds(0, HD)]
                pl.when((zz <= at[2]) & (at[2] < depth - 1))(lambda: sent_bytes(ref, z_send.at[p, 0, zz]))
                pl.when((zz >= at[2]) & (at[2] > 0))(lambda: sent_bytes(ref, z_send.at[p, 1, zz]))

            sent_bytes(full.at[p, core, :, pl.ds(0, half), pl.ds(0, seconds * HD)], s_send.at[p])
            sent_bytes(full.at[p, core, :, :, pl.ds(0, thirds * HD)], t_send.at[p])
            sent_bytes(full.at[p, core], c_send.at[p])


    def first_copies(p, zz, same):
        for h in range(2):
            d1, d2 = ORDER[h]
            part, r1, q1 = halves[h][0], halves[h][1], halves[h][6 + same]
            for k1 in range(1, dims[d1]):
                v1 = (at[d1] + k1) % dims[d1]
                for k2 in (0,) if same else range(1, dims[d2]):
                    v2 = (at[d2] + k2) % dims[d2]
                    send(part.at[p, zz, v1, v2], r1.at[p, k1 - 1, zz, v2], halves[h][5].at[p], q1.at[p, zz],
                         target(dims, at, core, d1, k1)).start()

    def take_first(p, h, zz, same):
        count = 1 if same else dims[ORDER[h][1]] - 1
        take_bytes(halves[h][1].at[p, :, zz, pl.ds(0, count)], halves[h][6 + same].at[p, zz])

    def swap_y(p):
        return send(y1.at[p], y2.at[p], y_send.at[p], y_recv.at[p], other)

    def partial_own(p):
        @pl.loop(0, depth)
        def _(zz):
            x = hid[:, pl.ds(pl.multiple_of((2 * zz + core) * rows, rows), rows)]
            early[zz] = mm(x, y1[p], TN)

    def turn(step):
        return (at[2] + step) % depth

    def partial_sum(p, zz):
        x = x2[:, pl.ds(pl.multiple_of(zz * rows, rows), rows)]
        r = (early[zz] + mm(x, y2[p], TN)).astype(jnp.bfloat16)
        for dp in range(across):
            where = (dp // dims[1], dp % dims[1])
            for h in range(2):
                d1, d2 = ORDER[h]
                halves[h][0][p, zz, where[d1], where[d2]] = (
                    r[h * half:(h + 1) * half, dp * HD:(dp + 1) * HD])

    def keep1(p, h, zz, v2):
        d1, d2 = ORDER[h]
        part, r1 = halves[h][0], halves[h][1]
        total = part[p, zz, at[d1], v2].astype(jnp.float32)
        for k1 in range(1, dims[d1]):
            total += r1[p, k1 - 1, zz, v2].astype(jnp.float32)
        return total

    def sum_second(p, zz):
        for h in range(2):
            d2 = ORDER[h][1]
            sum2, r2 = halves[h][2], halves[h][3]
            take_first(p, h, zz, 0)
            for k2 in range(1, dims[d2]):
                v2 = (at[d2] + k2) % dims[d2]
                sum2[p, k2 - 1, zz] = keep1(p, h, zz, v2).astype(jnp.bfloat16)
                send(sum2.at[p, k2 - 1, zz], r2.at[p, k2 - 1, zz], halves[h][8].at[p], halves[h][9].at[p, zz],
                     target(dims, at, core, d2, k2)).start()

    def keep2(p, h, zz):
        d2 = ORDER[h][1]
        take_first(p, h, zz, 1)
        total = keep1(p, h, zz, at[d2])
        take_bytes(halves[h][3].at[p, :, zz], halves[h][9].at[p, zz])
        for k2 in range(1, dims[d2]):
            total += halves[h][3][p, k2 - 1, zz].astype(jnp.float32)
        return total

    def sum_third(p, step):
        zz = turn(step)
        for h in range(2):
            d1, d2 = ORDER[h]
            part, r3 = halves[h][0], halves[h][4]
            part[p, zz, at[d1], at[d2]] = keep2(p, h, zz).astype(jnp.bfloat16)
            send(part.at[p, zz, at[d1], at[d2]], r3.at[p, step - 1], halves[h][10].at[p], halves[h][11].at[p],
                 target(dims, at, core, 2, step)).start()

    def finish(p):
        for h in range(2):
            total = keep2(p, h, at[2])
            take_bytes(halves[h][4].at[p], halves[h][11].at[p])
            for k in range(1, depth):
                total += halves[h][4][p, k - 1].astype(jnp.float32)
            grad[h * half:(h + 1) * half, p * HD:(p + 1) * HD] = total

    def drain_reduce(p):
        for h in range(2):
            sent_bytes(halves[h][1].at[p], halves[h][5].at[p])
            sent_bytes(halves[h][3].at[p], halves[h][8].at[p])
            sent_bytes(halves[h][4].at[p], halves[h][10].at[p])


    points = [pltpu.make_async_copy(ref, pts.at[i], load_sem.at[i])
              for i, ref in enumerate((start_ref, mid_ref, end_ref))]
    wholes = [pltpu.make_async_copy(ref, dst, load_sem.at[3 + i])
              for i, (ref, dst) in enumerate(((hidden_ref, hid), (query_ref, qv), (cot_ref, gv)))]
    for load in points + wholes:
        load.start()
    barrier = pltpu.get_barrier_semaphore()
    peers = all_peers(dims, at, core)
    for peer in peers:
        pl.semaphore_signal(barrier, inc=1, device_id=peer, device_id_type=MESH)
    for load in points:
        load.wait()
    t_value = t_ref[0]
    blended = (
        (1.0 - t_value) * (1.0 - t_value) * pts[0].astype(jnp.float32)
        + 2.0 * t_value * (1.0 - t_value) * pts[1].astype(jnp.float32)
        + t_value * t_value * pts[2].astype(jnp.float32)
    ).astype(jnp.bfloat16)
    col = pl.multiple_of((at[0] * dims[1] + at[1]) * HD, HD)
    for p in range(groups):
        full[p, core, at[2], :, pl.ds(col, HD)] = blended[:, p * HD:(p + 1) * HD]
    pl.semaphore_wait(barrier, len(peers))

    def send_both(p, zz):
        for h in range(2):
            send_all(p, h, zz)

    own_z(0)
    for p in range(min(groups, 2)):
        send_both(p, at[2])

    @pl.loop(0, depth)
    def _(zz):
        swap_x(zz).start()

    cosine, sine_t = rope_tables(*cos_ref.shape)
    cos_ref[...] = cosine
    sin_ref[...] = sine_t

    def take_first_group(k):
        near(k, lambda zz, side: take_z(0, zz, side))

    def relay_first_group(k):
        near(k, lambda zz, side: relay_second(0, zz))

    take_first_group(1)
    relay_second(0, at[2])

    @pl.loop(2, depth)
    def _(k):
        take_first_group(k)
        if groups > 1:
            pl.when(k == depth - 2)(lambda: own_z(1))
        relay_first_group(k - 1)

    wholes[0].wait()
    if groups > 1:
        near(1, lambda zz, side: take_z(1, zz, side, False))
    third(0, at[2], True)
    relay_first_group(depth - 1)
    if groups > 1:
        near(1, lambda zz, side: send_both(1, zz))
    near(1, lambda zz, side: third(0, zz))
    from_core(0, at[2])

    @pl.loop(2, depth)
    def _(k):
        if groups > 1:
            pl.when(k < depth - 1)(lambda: near(k, lambda zz, side: take_z(1, zz, side)))
        near(k, lambda zz, side: third(0, zz))
        near(k - 1, lambda zz, side: from_core(0, zz))

    near(depth - 1, lambda zz, side: from_core(0, zz))
    if groups > 1:
        near(depth - 1, lambda zz, side: take_z(1, zz, side))
    wholes[1].wait()
    wholes[2].wait()

    def around(act):
        @pl.loop(0, depth)
        def _(i):
            act(turn(i))

    share = depth // heads
    early_steps = min(2, depth - 1)
    for p in range(groups):
        if p > 0:
            around(lambda zz: third(p, zz))
            around(lambda zz: from_core(p, zz))

            @pl.loop(1, early_steps + 1)
            def _(step):
                sum_second(p - 1, turn(step))

            @pl.loop(1, early_steps + 1)
            def _(step):
                first_copies(p - 1, turn(step), 1)
        kv[...] = acc[...].astype(jnp.bfloat16)
        if p < last:
            acc[...] = jnp.zeros_like(acc)

        @pl.loop(0, heads)
        def _(d):
            keys_at = pl.ds(pl.multiple_of(d * HD, HD), HD)
            values_at = pl.ds(pl.multiple_of((heads + d) * HD, HD), HD)
            width = qv.shape[1] // (heads * groups)
            attend_head(keys_at, values_at, ((d * groups + p) * width, width), kv, qv, gv, cos_ref,
                        sin_ref, ctx, y1.at[p], kg, vg)
            if p < last:
                @pl.loop(0, share)
                def _(i):
                    k = d * share + i
                    pl.when(k == 0)(lambda: relay_second(p + 1, at[2]))
                    pl.when(k > 0)(lambda: near(k, lambda zz, side: relay_second(p + 1, zz)))
            if p > 0:
                @pl.when(d == 0)
                def _():
                    @pl.loop(early_steps + 1, depth + 1)
                    def _(step):
                        sum_second(p - 1, turn(step))
                        first_copies(p - 1, turn(step), 1)

        swap_y(p).start()
        if p > 0:
            @pl.loop(1, early_steps + 1)
            def _(step):
                sum_third(p - 1, step)
        partial_own(p)
        if p == 0:
            take_bytes(x2, x_recv.at[0])
        swap_y(p).wait()
        if p < last:
            @pl.loop(1, depth + 1)
            def _(step):
                partial_sum(p, turn(step))
                first_copies(p, turn(step), 0)

    partial_sum(last, turn(1))
    first_copies(last, turn(1), 0)
    partial_sum(last, turn(2))
    first_copies(last, turn(2), 0)
    first_copies(last, turn(1), 1)

    @pl.loop(3, depth + 1)
    def _(step):
        partial_sum(last, turn(step))

    for p in range(last):
        @pl.loop(early_steps + 1, depth)
        def _(step):
            sum_third(p, step)

    sum_second(last, turn(1))
    first_copies(last, turn(2), 1)
    sum_second(last, turn(2))

    @pl.loop(3, depth)
    def _(step):
        first_copies(last, turn(step), 0)
        first_copies(last, turn(step), 1)

    first_copies(last, at[2], 0)
    for p in range(last):
        finish(p)
    drain_gather()
    sent_bytes(x2, x_send.at[0])

    @pl.loop(1, depth - 1)
    def _(step):
        sum_third(last, step)

    @pl.loop(3, depth)
    def _(step):
        sum_second(last, turn(step))

    first_copies(last, at[2], 1)
    sum_second(last, at[2])
    sum_third(last, depth - 1)
    for p in range(last):
        drain_reduce(p)
    finish(last)
    drain_reduce(last)


def run_step(dims, hidden, queries, cotangent, point_start, point_mid, point_end, curve_time):
    rows, cols = point_mid.shape
    seq = hidden.shape[0]
    a, b, z = dims
    groups = cols // HD
    half = rows // 2
    width = a * b * HD
    sem = pltpu.SemaphoreType.DMA

    def vm(*shape, dtype=jnp.bfloat16):
        return pltpu.VMEM(shape, dtype)

    f32 = jnp.float32
    scratch = [
        vm(3, rows, cols), vm(*hidden.shape), vm(seq, z * rows),
        vm(*queries.shape), vm(*cotangent.shape),
        vm(seq, HD, dtype=f32), vm(seq, HD, dtype=f32),
        vm(groups, 2, z, rows, width), vm(seq, width, dtype=f32), vm(seq, width),
        vm(seq, HD, dtype=f32), vm(seq, HD, dtype=f32),
        vm(groups, seq, width), vm(groups, seq, width), vm(z, rows, width, dtype=f32),
        sem((6,)), sem((1,)), sem((1,)), sem((groups,)), sem((groups,)),
        sem((groups, 2, z)), sem((groups,)), sem((groups,)), sem((groups,)),
        sem((groups, 2, z)), sem((groups, 2, z)), sem((groups, z)),
    ]
    scratch += [sem((groups, z, dims[ORDER[1 - h][0]] - 1)) for h in range(2)]
    for h in range(2):
        n1, n2 = dims[ORDER[h][0]], dims[ORDER[h][1]]
        scratch += [
            vm(groups, z, n1, n2, half, HD), vm(groups, n1 - 1, z, n2, half, HD),
            vm(groups, n2 - 1, z, half, HD), vm(groups, n2 - 1, z, half, HD),
            vm(groups, z - 1, half, HD),
            sem((groups,)), sem((groups, z)), sem((groups, z)),
            sem((groups,)), sem((groups, z)),
            sem((groups,)), sem((groups,)),
        ]
    hbm = pl.BlockSpec(memory_space=pl.ANY)
    return pl.pallas_call(
        functools.partial(step_kernel, dims),
        out_shape=(
            pltpu.VMEM(queries.shape, jnp.bfloat16),
            pltpu.VMEM((rows, cols), f32),
        ),
        in_specs=[pl.BlockSpec(memory_space=pltpu.SMEM)] + [hbm] * 6,
        out_specs=(pl.BlockSpec(memory_space=pltpu.VMEM),) * 2,
        scratch_shapes=scratch,
        compiler_params=pltpu.CompilerParams(
            collective_id=1, has_side_effects=True, vmem_limit_bytes=VMEM_LIMIT),
        name="bezier_step",
    )(curve_time, point_start, point_mid, point_end, hidden, queries, cotangent)


def local(dims, hidden, queries, cotangent, point_start, point_mid, point_end, curve_time):
    t_value = curve_time[0]
    context, gradient = run_step(dims, hidden, queries, cotangent, point_start, point_mid, point_end, curve_time)
    return (context, gradient * (2.0 * t_value * (1.0 - t_value)))


def solution(mesh):
    dp, fsdp = mesh.shape["dp"], mesh.shape["fsdp"]
    dims = (dp // 2, 2, fsdp // 2)
    return jax.shard_map(
        functools.partial(local, dims),
        mesh=mesh,
        in_specs=(
            P(("dp", "fsdp"), None),
            P(("dp", "fsdp"), None),
            P(("dp", "fsdp"), None),
            P("fsdp", "dp"),
            P("fsdp", "dp"),
            P("fsdp", "dp"),
            P(),
        ),
        out_specs=(P(("dp", "fsdp"), None), P("fsdp", "dp")),
        check_vma=False,
    )
```

```python
import functools
import math

import jax
import jax.numpy as jnp
from jax import lax
from jax.experimental import pallas as pl
from jax.experimental.pallas import tpu as pltpu
from jax.sharding import PartitionSpec as P

HD = 128
BQ = 256
MESH = pl.DeviceIdType.MESH
VMEM_LIMIT = 60 * 1024 * 1024


def rope_tables(seq_len, head_dim):
    shape = (seq_len, head_dim)
    positions = lax.broadcasted_iota(jnp.int32, shape, 0).astype(jnp.float32)
    column = lax.broadcasted_iota(jnp.int32, shape, 1)
    halves_index = jnp.where(column < head_dim // 2, column, column - head_dim // 2).astype(jnp.float32)
    inverse = jnp.exp(-(2.0 * halves_index / head_dim) * math.log(500000.0))
    angles = positions * inverse
    cosine, sine_t = jnp.cos(angles), jnp.sin(angles)
    return (cosine, sine_t)


def rotate(x):
    half = x.shape[-1] // 2
    return jnp.concatenate([-x[..., half:], x[..., :half]], axis=-1)


def rotate_back(x):
    half = x.shape[-1] // 2
    return jnp.concatenate([x[..., half:], -x[..., :half]], axis=-1)


NN = (((1,), (0,)), ((), ()))
NT = (((1,), (1,)), ((), ()))
TN = (((0,), (0,)), ((), ()))


def mm(x, y, dims=NN):
    return lax.dot_general(x, y, dims, preferred_element_type=jnp.float32)


ORDER = ((1, 0), (0, 1))


def place(dims):
    dp, fs = lax.axis_index("dp"), lax.axis_index("fsdp")
    return (dp // dims[1], dp % dims[1], fs // 2), fs % 2


def target(dims, at, core, axis=None, offset=0):
    at = list(at)
    if axis is not None:
        at[axis] = (at[axis] + offset + dims[axis]) % dims[axis]
    return (at[0] * dims[1] + at[1], at[2] * 2 + core)


def send(src, dst, send_sem, recv_sem, peer):
    return pltpu.make_async_remote_copy(
        src_ref=src, dst_ref=dst, send_sem=send_sem, recv_sem=recv_sem,
        device_id=peer, device_id_type=MESH)


def all_peers(dims, at, core):
    peers = [target(dims, at, core, axis, k) for axis in range(3) for k in range(1, dims[axis])]
    return peers + [target(dims, at, 1 - core)]


def attend_head(keys_at, values_at, q_cols, kv, q_ref, g_ref, cos_ref, sin_ref, ctx_ref, y_ref, kg, vg):
    seq = kv.shape[0]
    group = q_cols[1] // HD
    scale = 1.0 / math.sqrt(HD)
    to_base2 = scale * math.log2(math.e)

    def cols(g):
        return pl.ds(pl.multiple_of(q_cols[0] + g * HD, HD), HD)

    raw = kv[:, keys_at].astype(jnp.float32)
    cosine, sine_t = cos_ref[...], sin_ref[...]
    keys = (raw * cosine + rotate(raw) * sine_t).astype(jnp.bfloat16)
    values = kv[:, values_at]
    values_t = values.astype(jnp.float32).T.astype(jnp.bfloat16)
    kg[...] = jnp.zeros_like(kg)
    vg[...] = jnp.zeros_like(vg)
    for start in range(0, seq, BQ):
        nk = start + BQ
        rows = slice(start, nk)
        qs = jnp.concatenate([q_ref[rows, cols(g)] for g in range(group)], axis=0)
        gs = jnp.concatenate([g_ref[rows, cols(g)] for g in range(group)], axis=0)
        s = mm(keys[:nk], qs, NT)
        key_at = lax.broadcasted_iota(jnp.int32, (BQ, group * BQ), 0)
        query_at = lax.broadcasted_iota(jnp.int32, (BQ, group * BQ), 1) % BQ
        last = jnp.where(key_at <= query_at, s[start:], -1e30)
        s = last if start == 0 else jnp.concatenate([s[:start], last], axis=0)
        top = jnp.max(s, axis=0, keepdims=True)
        w = jnp.exp2((s - top) * to_base2)
        p = w * (1.0 / jnp.sum(w, axis=0, keepdims=True))
        p_low = p.astype(jnp.bfloat16)
        ctx_t = mm(values_t[:, :nk], p_low)
        dp = mm(values[:nk], gs, NT)
        vg[:nk] += mm(p_low, gs)
        delta = jnp.sum(dp * p, axis=0, keepdims=True)
        ds = (p * ((dp - delta) * scale)).astype(jnp.bfloat16)
        kg[:nk] += mm(ds, qs)
        ctx = ctx_t.T.astype(jnp.bfloat16)
        for g in range(group):
            ctx_ref[rows, cols(g)] = ctx[g * BQ:(g + 1) * BQ]
    rot = kg[...]
    y_ref[:, keys_at] = (rot * cosine + rotate_back(rot * sine_t)).astype(jnp.bfloat16)
    y_ref[:, values_at] = vg[...].astype(jnp.bfloat16)


def step_kernel(dims, t_ref, start_ref, mid_ref, end_ref, hidden_ref, query_ref, cot_ref, ctx, grad,
                pts, hid, x2, qv, gv, cos_ref, sin_ref, full, acc, kv, kg, vg, y1, y2, early,
                load_sem, x_send, x_recv, y_send, y_recv, z_send, s_send, t_send, c_send,
                z_recv, t_recv, c_recv, *more):
    s_recv = more[:2]
    halves = [more[2:14], more[14:26]]
    at, core = place(dims)
    depth = dims[2]
    across = dims[0] * dims[1]
    rows = start_ref.shape[0]
    half = rows // 2
    groups = full.shape[0]
    last = groups - 1
    heads = across // 2
    other = target(dims, at, 1 - core)
    here = at[:2]

    def take_bytes(ref, sem):
        send(ref, ref, c_send.at[0], sem, other).wait_recv()

    def sent_bytes(ref, sem):
        send(ref, ref, sem, c_recv.at[0, 0], other).wait_send()


    def piece(p, c, h, zz, pos):
        col = pl.multiple_of((pos[0] * dims[1] + pos[1]) * HD, HD)
        return full.at[p, c, zz, pl.ds(h * half, half), pl.ds(col, HD)]

    def moved(axis, k):
        pos = [at[0], at[1]]
        pos[axis] = (pos[axis] + k) % dims[axis]
        return pos

    def push(p, h, zz, pos, send_sem, recv_sem, peer):
        ref = piece(p, core, h, zz, pos)
        return send(ref, ref, send_sem, recv_sem, peer)

    def near(k, act):
        @pl.loop(0, 2)
        def _(side):
            zz = at[2] + (2 * side - 1) * k
            pl.when((zz >= 0) & (zz < depth))(lambda: act(zz, side))

    def to_z(p, h, zz, side):
        push(p, h, zz, here, z_send.at[p, side, zz], z_recv.at[p, h, zz],
             target(dims, at, core, 2, 1 - 2 * side)).start()

    def onward(side):
        return ((side == 0) & (at[2] < depth - 1)) | ((side == 1) & (at[2] > 0))

    def to_second(p, h, zz, k):
        push(p, h, zz, here, s_send.at[p], s_recv[h].at[p, zz, k - 1],
             target(dims, at, core, ORDER[1 - h][0], k)).start()

    def to_third(p, h, zz, pos, k):
        push(p, h, zz, pos, t_send.at[p], t_recv.at[p, h, zz],
             target(dims, at, core, ORDER[1 - h][1], k)).start()

    def to_core(p, h, zz, pos):
        push(p, h, zz, pos, c_send.at[p], c_recv.at[p, zz], other).start()

    def swap_x(zz):
        src = pl.multiple_of((2 * zz + 1 - core) * rows, rows)
        dst = pl.multiple_of(zz * rows, rows)
        return send(hidden_ref.at[:, pl.ds(src, rows)], x2.at[:, pl.ds(dst, rows)],
                    x_send.at[0], x_recv.at[0], other)

    def own_z(p):
        @pl.loop(0, 2)
        def _(side):
            @pl.when(onward(side))
            def _():
                for h in range(2):
                    to_z(p, h, at[2], side)

    def send_all(p, h, zz):
        for k in range(1, dims[ORDER[1 - h][0]]):
            to_second(p, h, zz, k)
        for k in range(1, dims[ORDER[1 - h][1]]):
            to_third(p, h, zz, here, k)
        to_core(p, h, zz, here)

    def take_z(p, zz, side, more=True):
        for h in range(2):
            take_bytes(piece(p, core, h, zz, here), z_recv.at[p, h, zz])
            pl.when(onward(side))(lambda: to_z(p, h, zz, side))
            if more:
                send_all(p, h, zz)

    def relay_second(p, zz):
        for h in range(2):
            d2, d3 = ORDER[1 - h]
            for k2 in range(1, dims[d2]):
                pos = moved(d2, k2)
                take_bytes(piece(p, core, h, zz, pos), s_recv[h].at[p, zz, dims[d2] - k2 - 1])
                for k in range(1, dims[d3]):
                    to_third(p, h, zz, pos, k)
                to_core(p, h, zz, pos)

    def product(p, c, zz, first=False):
        x = hid[:, pl.ds(pl.multiple_of((2 * zz + c) * rows, rows), rows)]
        got = mm(x, full[p, c, zz])
        if first:
            acc[...] = got
        else:
            acc[...] += got

    def third(p, zz, first=False):
        for h in range(2):
            d2, d3 = ORDER[1 - h]
            count = (dims[d3] - 1) * dims[d2]
            take_bytes(full.at[p, core, zz, pl.ds(0, half), pl.ds(0, count * HD)], t_recv.at[p, h, zz])
            for k3 in range(1, dims[d3]):
                for k2 in range(dims[d2]):
                    pos = moved(d3, k3)
                    pos[d2] = (at[d2] + k2) % dims[d2]
                    to_core(p, h, zz, pos)
        product(p, core, zz, first)

    def from_core(p, zz):
        take_bytes(full.at[p, 1 - core, zz], c_recv.at[p, zz])
        product(p, 1 - core, zz)

    def drain_gather():
        seconds = dims[0] + dims[1] - 2
        thirds = (2 * across - dims[0] - dims[1]) // 2
        for p in range(groups):
            @pl.loop(0, depth)
            def _(zz):
                ref = full.at[p, core, zz, :, pl.ds(0, HD)]
                pl.when((zz <= at[2]) & (at[2] < depth - 1))(lambda: sent_bytes(ref, z_send.at[p, 0, zz]))
                pl.when((zz >= at[2]) & (at[2] > 0))(lambda: sent_bytes(ref, z_send.at[p, 1, zz]))

            sent_bytes(full.at[p, core, :, pl.ds(0, half), pl.ds(0, seconds * HD)], s_send.at[p])
            sent_bytes(full.at[p, core, :, :, pl.ds(0, thirds * HD)], t_send.at[p])
            sent_bytes(full.at[p, core], c_send.at[p])


    def first_copies(p, zz, same):
        for h in range(2):
            d1, d2 = ORDER[h]
            part, r1, q1 = halves[h][0], halves[h][1], halves[h][6 + same]
            for k1 in range(1, dims[d1]):
                v1 = (at[d1] + k1) % dims[d1]
                for k2 in (0,) if same else range(1, dims[d2]):
                    v2 = (at[d2] + k2) % dims[d2]
                    send(part.at[p, zz, v1, v2], r1.at[p, k1 - 1, zz, v2], halves[h][5].at[p], q1.at[p, zz],
                         target(dims, at, core, d1, k1)).start()

    def take_first(p, h, zz, same):
        count = 1 if same else dims[ORDER[h][1]] - 1
        take_bytes(halves[h][1].at[p, :, zz, pl.ds(0, count)], halves[h][6 + same].at[p, zz])

    def swap_y(p, columns):
        send(y1.at[p, :, columns], y2.at[p, :, columns], y_send.at[p], y_recv.at[p], other).start()

    def partial_own(p, zz):
        x = hid[:, pl.ds(pl.multiple_of((2 * zz + core) * rows, rows), rows)]
        early[zz] = mm(x, y1[p], TN)

    def turn(step):
        return (at[2] + step) % depth

    def partial_sum(p, zz):
        x = x2[:, pl.ds(pl.multiple_of(zz * rows, rows), rows)]
        r = (early[zz] + mm(x, y2[p], TN)).astype(jnp.bfloat16)
        for dp in range(across):
            where = (dp // dims[1], dp % dims[1])
            for h in range(2):
                d1, d2 = ORDER[h]
                halves[h][0][p, zz, where[d1], where[d2]] = (
                    r[h * half:(h + 1) * half, dp * HD:(dp + 1) * HD])

    def keep1(p, h, zz, v2):
        d1, d2 = ORDER[h]
        part, r1 = halves[h][0], halves[h][1]
        total = part[p, zz, at[d1], v2].astype(jnp.float32)
        for k1 in range(1, dims[d1]):
            total += r1[p, k1 - 1, zz, v2].astype(jnp.float32)
        return total

    def sum_second(p, zz):
        for h in range(2):
            d2 = ORDER[h][1]
            sum2, r2 = halves[h][2], halves[h][3]
            take_first(p, h, zz, 0)
            for k2 in range(1, dims[d2]):
                v2 = (at[d2] + k2) % dims[d2]
                sum2[p, k2 - 1, zz] = keep1(p, h, zz, v2).astype(jnp.bfloat16)
                send(sum2.at[p, k2 - 1, zz], r2.at[p, k2 - 1, zz], halves[h][8].at[p], halves[h][9].at[p, zz],
                     target(dims, at, core, d2, k2)).start()

    def keep2(p, h, zz):
        d2 = ORDER[h][1]
        take_first(p, h, zz, 1)
        total = keep1(p, h, zz, at[d2])
        take_bytes(halves[h][3].at[p, :, zz], halves[h][9].at[p, zz])
        for k2 in range(1, dims[d2]):
            total += halves[h][3][p, k2 - 1, zz].astype(jnp.float32)
        return total

    def sum_third(p, step):
        zz = turn(step)
        for h in range(2):
            d1, d2 = ORDER[h]
            part, r3 = halves[h][0], halves[h][4]
            part[p, zz, at[d1], at[d2]] = keep2(p, h, zz).astype(jnp.bfloat16)
            send(part.at[p, zz, at[d1], at[d2]], r3.at[p, step - 1], halves[h][10].at[p], halves[h][11].at[p],
                 target(dims, at, core, 2, step)).start()

    def finish(p):
        for h in range(2):
            total = keep2(p, h, at[2])
            take_bytes(halves[h][4].at[p], halves[h][11].at[p])
            for k in range(1, depth):
                total += halves[h][4][p, k - 1].astype(jnp.float32)
            grad[h * half:(h + 1) * half, p * HD:(p + 1) * HD] = total

    def drain_reduce(p):
        for h in range(2):
            sent_bytes(halves[h][1].at[p], halves[h][5].at[p])
            sent_bytes(halves[h][3].at[p], halves[h][8].at[p])
            sent_bytes(halves[h][4].at[p], halves[h][10].at[p])


    points = [pltpu.make_async_copy(ref, pts.at[i], load_sem.at[i])
              for i, ref in enumerate((start_ref, mid_ref, end_ref))]
    wholes = [pltpu.make_async_copy(ref, dst, load_sem.at[3 + i])
              for i, (ref, dst) in enumerate(((hidden_ref, hid), (query_ref, qv), (cot_ref, gv)))]
    for load in points + wholes:
        load.start()
    barrier = pltpu.get_barrier_semaphore()
    peers = all_peers(dims, at, core)
    for peer in peers:
        pl.semaphore_signal(barrier, inc=1, device_id=peer, device_id_type=MESH)
    for load in points:
        load.wait()
    t_value = t_ref[0]
    blended = (
        (1.0 - t_value) * (1.0 - t_value) * pts[0].astype(jnp.float32)
        + 2.0 * t_value * (1.0 - t_value) * pts[1].astype(jnp.float32)
        + t_value * t_value * pts[2].astype(jnp.float32)
    ).astype(jnp.bfloat16)
    col = pl.multiple_of((at[0] * dims[1] + at[1]) * HD, HD)
    for p in range(groups):
        full[p, core, at[2], :, pl.ds(col, HD)] = blended[:, p * HD:(p + 1) * HD]
    pl.semaphore_wait(barrier, len(peers))

    def send_both(p, zz):
        for h in range(2):
            send_all(p, h, zz)

    own_z(0)
    for p in range(min(groups, 2)):
        send_both(p, at[2])

    @pl.loop(0, depth)
    def _(zz):
        swap_x(zz).start()

    cosine, sine_t = rope_tables(*cos_ref.shape)
    cos_ref[...] = cosine
    sin_ref[...] = sine_t

    def take_first_group(k):
        near(k, lambda zz, side: take_z(0, zz, side))

    def relay_first_group(k):
        near(k, lambda zz, side: relay_second(0, zz))

    take_first_group(1)
    relay_second(0, at[2])

    @pl.loop(2, depth)
    def _(k):
        take_first_group(k)
        if groups > 1:
            pl.when(k == depth - 2)(lambda: own_z(1))
        relay_first_group(k - 1)

    wholes[0].wait()
    if groups > 1:
        near(1, lambda zz, side: take_z(1, zz, side, False))
    third(0, at[2], True)
    relay_first_group(depth - 1)
    if groups > 1:
        near(1, lambda zz, side: send_both(1, zz))
    near(1, lambda zz, side: third(0, zz))
    from_core(0, at[2])

    @pl.loop(2, depth)
    def _(k):
        if groups > 1:
            pl.when(k < depth - 1)(lambda: near(k, lambda zz, side: take_z(1, zz, side)))
        near(k, lambda zz, side: third(0, zz))
        near(k - 1, lambda zz, side: from_core(0, zz))

    near(depth - 1, lambda zz, side: from_core(0, zz))
    if groups > 1:
        near(depth - 1, lambda zz, side: take_z(1, zz, side))
    wholes[1].wait()
    wholes[2].wait()

    def around(act):
        @pl.loop(0, depth)
        def _(i):
            act(turn(i))

    share = depth // heads
    early_steps = min(2, depth - 1)
    for p in range(groups):
        if p > 0:
            around(lambda zz: third(p, zz))
            around(lambda zz: from_core(p, zz))

            @pl.loop(1, early_steps + 1)
            def _(step):
                sum_second(p - 1, turn(step))

            @pl.loop(1, early_steps + 1)
            def _(step):
                first_copies(p - 1, turn(step), 1)
        kv[...] = acc[...].astype(jnp.bfloat16)
        if p < last:
            acc[...] = jnp.zeros_like(acc)

        @pl.loop(0, heads)
        def _(d):
            keys_at = pl.ds(pl.multiple_of(d * HD, HD), HD)
            values_at = pl.ds(pl.multiple_of((heads + d) * HD, HD), HD)
            width = qv.shape[1] // (heads * groups)
            attend_head(keys_at, values_at, ((d * groups + p) * width, width), kv, qv, gv, cos_ref,
                        sin_ref, ctx, y1.at[p], kg, vg)
            swap_y(p, keys_at)
            swap_y(p, values_at)
            if p < last:
                @pl.loop(0, share)
                def _(i):
                    k = d * share + i
                    pl.when(k == 0)(lambda: relay_second(p + 1, at[2]))
                    pl.when(k > 0)(lambda: near(k, lambda zz, side: relay_second(p + 1, zz)))
            if p > 0:
                @pl.when(d == 0)
                def _():
                    @pl.loop(early_steps + 1, depth + 1)
                    def _(step):
                        sum_second(p - 1, turn(step))
                        first_copies(p - 1, turn(step), 1)

        if p > 0:
            @pl.loop(1, early_steps + 1)
            def _(step):
                sum_third(p - 1, step)
        partial_own(p, turn(1))
        partial_own(p, turn(2))
        if p == 0:
            take_bytes(x2, x_recv.at[0])
        take_bytes(y2.at[p], y_recv.at[p])
        if p < last:
            @pl.loop(1, depth + 1)
            def _(step):
                pl.when(step > 2)(lambda: partial_own(p, turn(step)))
                partial_sum(p, turn(step))
                first_copies(p, turn(step), 0)

    partial_sum(last, turn(1))
    first_copies(last, turn(1), 0)
    partial_sum(last, turn(2))
    first_copies(last, turn(2), 0)
    first_copies(last, turn(1), 1)

    @pl.loop(3, depth + 1)
    def _(step):
        partial_own(last, turn(step))
        partial_sum(last, turn(step))

    for p in range(last):
        @pl.loop(early_steps + 1, depth)
        def _(step):
            sum_third(p, step)

    sum_second(last, turn(1))
    first_copies(last, turn(2), 1)
    sum_second(last, turn(2))

    @pl.loop(3, depth)
    def _(step):
        first_copies(last, turn(step), 0)
        first_copies(last, turn(step), 1)

    first_copies(last, at[2], 0)
    drain_gather()
    sent_bytes(x2, x_send.at[0])

    @pl.loop(1, depth - 1)
    def _(step):
        sum_third(last, step)

    @pl.loop(3, depth)
    def _(step):
        sum_second(last, turn(step))

    first_copies(last, at[2], 1)
    sum_second(last, at[2])
    sum_third(last, depth - 1)
    for p in range(groups):
        sent_bytes(y1.at[p], y_send.at[p])
    for p in range(last):
        finish(p)
        drain_reduce(p)
    finish(last)
    drain_reduce(last)


def run_step(dims, hidden, queries, cotangent, point_start, point_mid, point_end, curve_time):
    rows, cols = point_mid.shape
    seq = hidden.shape[0]
    a, b, z = dims
    groups = cols // HD
    half = rows // 2
    width = a * b * HD
    sem = pltpu.SemaphoreType.DMA

    def vm(*shape, dtype=jnp.bfloat16):
        return pltpu.VMEM(shape, dtype)

    f32 = jnp.float32
    scratch = [
        vm(3, rows, cols), vm(*hidden.shape), vm(seq, z * rows),
        vm(*queries.shape), vm(*cotangent.shape),
        vm(seq, HD, dtype=f32), vm(seq, HD, dtype=f32),
        vm(groups, 2, z, rows, width), vm(seq, width, dtype=f32), vm(seq, width),
        vm(seq, HD, dtype=f32), vm(seq, HD, dtype=f32),
        vm(groups, seq, width), vm(groups, seq, width), vm(z, rows, width, dtype=f32),
        sem((6,)), sem((1,)), sem((1,)), sem((groups,)), sem((groups,)),
        sem((groups, 2, z)), sem((groups,)), sem((groups,)), sem((groups,)),
        sem((groups, 2, z)), sem((groups, 2, z)), sem((groups, z)),
    ]
    scratch += [sem((groups, z, dims[ORDER[1 - h][0]] - 1)) for h in range(2)]
    for h in range(2):
        n1, n2 = dims[ORDER[h][0]], dims[ORDER[h][1]]
        scratch += [
            vm(groups, z, n1, n2, half, HD), vm(groups, n1 - 1, z, n2, half, HD),
            vm(groups, n2 - 1, z, half, HD), vm(groups, n2 - 1, z, half, HD),
            vm(groups, z - 1, half, HD),
            sem((groups,)), sem((groups, z)), sem((groups, z)),
            sem((groups,)), sem((groups, z)),
            sem((groups,)), sem((groups,)),
        ]
    hbm = pl.BlockSpec(memory_space=pl.ANY)
    return pl.pallas_call(
        functools.partial(step_kernel, dims),
        out_shape=(
            pltpu.VMEM(queries.shape, jnp.bfloat16),
            pltpu.VMEM((rows, cols), f32),
        ),
        in_specs=[pl.BlockSpec(memory_space=pltpu.SMEM)] + [hbm] * 6,
        out_specs=(pl.BlockSpec(memory_space=pltpu.VMEM),) * 2,
        scratch_shapes=scratch,
        compiler_params=pltpu.CompilerParams(
            collective_id=1, has_side_effects=True, vmem_limit_bytes=VMEM_LIMIT),
        name="bezier_step",
    )(curve_time, point_start, point_mid, point_end, hidden, queries, cotangent)


def close_kernel(t_ref, ctx_ref, grad_ref, out_ctx, out_grad, scaled, sems):
    context = pltpu.make_async_copy(ctx_ref, out_ctx, sems.at[0])
    context.start()
    t_value = t_ref[0]
    scaled[...] = grad_ref[...] * (2.0 * t_value * (1.0 - t_value))
    gradient = pltpu.make_async_copy(scaled, out_grad, sems.at[1])
    gradient.start()
    context.wait()
    gradient.wait()


def close_step(curve_time, context, gradient):
    hbm = pl.BlockSpec(memory_space=pl.ANY)
    return pl.pallas_call(
        close_kernel,
        out_shape=(
            jax.ShapeDtypeStruct(context.shape, context.dtype),
            jax.ShapeDtypeStruct(gradient.shape, gradient.dtype),
        ),
        in_specs=[pl.BlockSpec(memory_space=pltpu.SMEM), hbm, pl.BlockSpec(memory_space=pltpu.VMEM)],
        out_specs=(hbm, hbm),
        scratch_shapes=[pltpu.VMEM(gradient.shape, gradient.dtype), pltpu.SemaphoreType.DMA((2,))],
        compiler_params=pltpu.CompilerParams(vmem_limit_bytes=8 * 1024 * 1024),
        name="close_step",
    )(curve_time, context, gradient)


def local(dims, hidden, queries, cotangent, point_start, point_mid, point_end, curve_time):
    return close_step(curve_time, *run_step(
        dims, hidden, queries, cotangent, point_start, point_mid, point_end, curve_time))


def solution(mesh):
    dp, fsdp = mesh.shape["dp"], mesh.shape["fsdp"]
    dims = (dp // 2, 2, fsdp // 2)
    return jax.shard_map(
        functools.partial(local, dims),
        mesh=mesh,
        in_specs=(
            P(("dp", "fsdp"), None),
            P(("dp", "fsdp"), None),
            P(("dp", "fsdp"), None),
            P("fsdp", "dp"),
            P("fsdp", "dp"),
            P("fsdp", "dp"),
            P(),
        ),
        out_specs=(P(("dp", "fsdp"), None), P("fsdp", "dp")),
        check_vma=False,
    )
```

```python
import functools
import math

import jax
import jax.numpy as jnp
from jax import lax
from jax.experimental import pallas as pl
from jax.experimental.pallas import tpu as pltpu
from jax.sharding import PartitionSpec as P

HD = 128
BQ = 256
MESH = pl.DeviceIdType.MESH
VMEM_LIMIT = 60 * 1024 * 1024


def rope_tables(seq_len, head_dim):
    shape = (seq_len, head_dim)
    positions = lax.broadcasted_iota(jnp.int32, shape, 0).astype(jnp.float32)
    column = lax.broadcasted_iota(jnp.int32, shape, 1)
    halves_index = jnp.where(column < head_dim // 2, column, column - head_dim // 2).astype(jnp.float32)
    inverse = jnp.exp(-(2.0 * halves_index / head_dim) * math.log(500000.0))
    angles = positions * inverse
    cosine, sine_t = jnp.cos(angles), jnp.sin(angles)
    return (cosine, sine_t)


def rotate(x):
    half = x.shape[-1] // 2
    return jnp.concatenate([-x[..., half:], x[..., :half]], axis=-1)


def rotate_back(x):
    half = x.shape[-1] // 2
    return jnp.concatenate([x[..., half:], -x[..., :half]], axis=-1)


NN = (((1,), (0,)), ((), ()))
NT = (((1,), (1,)), ((), ()))
TN = (((0,), (0,)), ((), ()))


def mm(x, y, dims=NN):
    return lax.dot_general(x, y, dims, preferred_element_type=jnp.float32)


ORDER = ((1, 0), (0, 1))


def place(dims):
    dp, fs = lax.axis_index("dp"), lax.axis_index("fsdp")
    return (dp // dims[1], dp % dims[1], fs // 2), fs % 2


def target(dims, at, core, axis=None, offset=0):
    at = list(at)
    if axis is not None:
        at[axis] = (at[axis] + offset + dims[axis]) % dims[axis]
    return (at[0] * dims[1] + at[1], at[2] * 2 + core)


def send(src, dst, send_sem, recv_sem, peer):
    return pltpu.make_async_remote_copy(
        src_ref=src, dst_ref=dst, send_sem=send_sem, recv_sem=recv_sem,
        device_id=peer, device_id_type=MESH)


def all_peers(dims, at, core):
    peers = [target(dims, at, core, axis, k) for axis in range(3) for k in range(1, dims[axis])]
    return peers + [target(dims, at, 1 - core)]


def attend_head(keys_at, values_at, q_cols, kv, q_ref, g_ref, cos_ref, sin_ref, ctx_ref, y_ref, kg, vg):
    seq = kv.shape[0]
    group = q_cols[1] // HD
    scale = 1.0 / math.sqrt(HD)
    to_base2 = scale * math.log2(math.e)

    def cols(g):
        return pl.ds(pl.multiple_of(q_cols[0] + g * HD, HD), HD)

    raw = kv[:, keys_at].astype(jnp.float32)
    cosine, sine_t = cos_ref[...], sin_ref[...]
    keys = (raw * cosine + rotate(raw) * sine_t).astype(jnp.bfloat16)
    values = kv[:, values_at]
    values_t = values.astype(jnp.float32).T.astype(jnp.bfloat16)
    kg[...] = jnp.zeros_like(kg)
    vg[...] = jnp.zeros_like(vg)
    for start in range(0, seq, BQ):
        nk = start + BQ
        rows = slice(start, nk)
        qs = jnp.concatenate([q_ref[rows, cols(g)] for g in range(group)], axis=0)
        gs = jnp.concatenate([g_ref[rows, cols(g)] for g in range(group)], axis=0)
        s = mm(keys[:nk], qs, NT)
        key_at = lax.broadcasted_iota(jnp.int32, (BQ, group * BQ), 0)
        query_at = lax.broadcasted_iota(jnp.int32, (BQ, group * BQ), 1) % BQ
        last = jnp.where(key_at <= query_at, s[start:], -1e30)
        s = last if start == 0 else jnp.concatenate([s[:start], last], axis=0)
        top = jnp.max(s, axis=0, keepdims=True)
        w = jnp.exp2((s - top) * to_base2)
        p = w * (1.0 / jnp.sum(w, axis=0, keepdims=True))
        p_low = p.astype(jnp.bfloat16)
        ctx_t = mm(values_t[:, :nk], p_low)
        dp = mm(values[:nk], gs, NT)
        vg[:nk] += mm(p_low, gs)
        delta = jnp.sum(dp * p, axis=0, keepdims=True)
        ds = (p * ((dp - delta) * scale)).astype(jnp.bfloat16)
        kg[:nk] += mm(ds, qs)
        ctx = ctx_t.T.astype(jnp.bfloat16)
        for g in range(group):
            ctx_ref[rows, cols(g)] = ctx[g * BQ:(g + 1) * BQ]
    rot = kg[...]
    y_ref[:, keys_at] = (rot * cosine + rotate_back(rot * sine_t)).astype(jnp.bfloat16)
    y_ref[:, values_at] = vg[...].astype(jnp.bfloat16)


def step_kernel(dims, t_ref, start_ref, mid_ref, end_ref, hidden_ref, query_ref, cot_ref, ctx, grad,
                pts, hid, x2, qv, gv, cos_ref, sin_ref, full, acc, kv, kg, vg, y1, y2, early,
                load_sem, x_send, x_recv, y_send, y_recv, z_send, s_send, t_send, c_send,
                z_recv, t_recv, c_recv, same_recv, rest_recv, second_recv, *more):
    s_recv = more[:2]
    halves = [more[2:11], more[11:20]]
    at, core = place(dims)
    depth = dims[2]
    across = dims[0] * dims[1]
    rows = start_ref.shape[0]
    half = rows // 2
    groups = full.shape[0]
    last = groups - 1
    heads = across // 2
    other = target(dims, at, 1 - core)
    here = at[:2]

    def take_bytes(ref, sem):
        send(ref, ref, c_send.at[0], sem, other).wait_recv()

    def sent_bytes(ref, sem):
        send(ref, ref, sem, c_recv.at[0, 0], other).wait_send()


    def piece(p, c, h, zz, pos):
        col = pl.multiple_of((pos[0] * dims[1] + pos[1]) * HD, HD)
        return full.at[p, c, zz, pl.ds(h * half, half), pl.ds(col, HD)]

    def moved(axis, k):
        pos = [at[0], at[1]]
        pos[axis] = (pos[axis] + k) % dims[axis]
        return pos

    def push(p, h, zz, pos, send_sem, recv_sem, peer):
        ref = piece(p, core, h, zz, pos)
        return send(ref, ref, send_sem, recv_sem, peer)

    def near(k, act):
        @pl.loop(0, 2)
        def _(side):
            zz = at[2] + (2 * side - 1) * k
            pl.when((zz >= 0) & (zz < depth))(lambda: act(zz, side))

    def to_z(p, h, zz, side):
        push(p, h, zz, here, z_send.at[p, side, zz], z_recv.at[p, h, zz],
             target(dims, at, core, 2, 1 - 2 * side)).start()

    def onward(side):
        return ((side == 0) & (at[2] < depth - 1)) | ((side == 1) & (at[2] > 0))

    def to_second(p, h, zz, k):
        push(p, h, zz, here, s_send.at[p], s_recv[h].at[p, zz, k - 1],
             target(dims, at, core, ORDER[1 - h][0], k)).start()

    def to_third(p, h, zz, pos, k):
        push(p, h, zz, pos, t_send.at[p], t_recv.at[p, h, zz],
             target(dims, at, core, ORDER[1 - h][1], k)).start()

    def to_core(p, h, zz, pos):
        push(p, h, zz, pos, c_send.at[p], c_recv.at[p, zz], other).start()

    def swap_x(zz):
        src = pl.multiple_of((2 * zz + 1 - core) * rows, rows)
        dst = pl.multiple_of(zz * rows, rows)
        return send(hidden_ref.at[:, pl.ds(src, rows)], x2.at[:, pl.ds(dst, rows)],
                    x_send.at[0], x_recv.at[0], other)

    def own_z(p):
        @pl.loop(0, 2)
        def _(side):
            @pl.when(onward(side))
            def _():
                for h in range(2):
                    to_z(p, h, at[2], side)

    def send_all(p, h, zz):
        for k in range(1, dims[ORDER[1 - h][0]]):
            to_second(p, h, zz, k)
        for k in range(1, dims[ORDER[1 - h][1]]):
            to_third(p, h, zz, here, k)
        to_core(p, h, zz, here)

    def take_z(p, zz, side, more=True):
        for h in range(2):
            take_bytes(piece(p, core, h, zz, here), z_recv.at[p, h, zz])
            pl.when(onward(side))(lambda: to_z(p, h, zz, side))
            if more:
                send_all(p, h, zz)

    def relay_second(p, zz):
        for h in range(2):
            d2, d3 = ORDER[1 - h]
            for k2 in range(1, dims[d2]):
                pos = moved(d2, k2)
                take_bytes(piece(p, core, h, zz, pos), s_recv[h].at[p, zz, dims[d2] - k2 - 1])
                for k in range(1, dims[d3]):
                    to_third(p, h, zz, pos, k)
                to_core(p, h, zz, pos)

    def product(p, c, zz, first=False):
        x = hid[:, pl.ds(pl.multiple_of((2 * zz + c) * rows, rows), rows)]
        got = mm(x, full[p, c, zz])
        if first:
            acc[...] = got
        else:
            acc[...] += got

    def third(p, zz, first=False):
        for h in range(2):
            d2, d3 = ORDER[1 - h]
            count = (dims[d3] - 1) * dims[d2]
            take_bytes(full.at[p, core, zz, pl.ds(0, half), pl.ds(0, count * HD)], t_recv.at[p, h, zz])
            for k3 in range(1, dims[d3]):
                for k2 in range(dims[d2]):
                    pos = moved(d3, k3)
                    pos[d2] = (at[d2] + k2) % dims[d2]
                    to_core(p, h, zz, pos)
        product(p, core, zz, first)

    def from_core(p, zz):
        take_bytes(full.at[p, 1 - core, zz], c_recv.at[p, zz])
        product(p, 1 - core, zz)

    def drain_gather():
        seconds = dims[0] + dims[1] - 2
        thirds = (2 * across - dims[0] - dims[1]) // 2
        for p in range(groups):
            @pl.loop(0, depth)
            def _(zz):
                ref = full.at[p, core, zz, :, pl.ds(0, HD)]
                pl.when((zz <= at[2]) & (at[2] < depth - 1))(lambda: sent_bytes(ref, z_send.at[p, 0, zz]))
                pl.when((zz >= at[2]) & (at[2] > 0))(lambda: sent_bytes(ref, z_send.at[p, 1, zz]))

            sent_bytes(full.at[p, core, :, pl.ds(0, half), pl.ds(0, seconds * HD)], s_send.at[p])
            sent_bytes(full.at[p, core, :, :, pl.ds(0, thirds * HD)], t_send.at[p])
            sent_bytes(full.at[p, core], c_send.at[p])


    def cut(p):
        return 2 if p == last else 1

    def sub(p, r):
        size = half // cut(p)
        return pl.ds(pl.multiple_of(r * size, size), size)

    def take_pieces(p, count, sem):
        take_bytes(full.at[0, core, 0, pl.ds(0, half // cut(p)), pl.ds(0, count * HD)], sem)

    def first_copies(p, zz, r, same):
        for h in range(2):
            d1, d2 = ORDER[h]
            part, r1 = halves[h][0], halves[h][1]
            sem = (same_recv if same else rest_recv).at[p, zz, r]
            for k1 in range(1, dims[d1]):
                v1 = (at[d1] + k1) % dims[d1]
                for k2 in (0,) if same else range(1, dims[d2]):
                    v2 = (at[d2] + k2) % dims[d2]
                    send(part.at[p, zz, v1, v2, sub(p, r)], r1.at[p, k1 - 1, zz, v2, sub(p, r)],
                         halves[h][5].at[p], sem, target(dims, at, core, d1, k1)).start()

    def swap_y(p, columns):
        send(y1.at[p, :, columns], y2.at[p, :, columns], y_send.at[p], y_recv.at[p], other).start()

    def partial_own(p, zz):
        x = hid[:, pl.ds(pl.multiple_of((2 * zz + core) * rows, rows), rows)]
        early[zz] = mm(x, y1[p], TN)

    def turn(step):
        return (at[2] + step) % depth

    def partial_sum(p, zz):
        x = x2[:, pl.ds(pl.multiple_of(zz * rows, rows), rows)]
        r = (early[zz] + mm(x, y2[p], TN)).astype(jnp.bfloat16)
        for dp in range(across):
            where = (dp // dims[1], dp % dims[1])
            for h in range(2):
                d1, d2 = ORDER[h]
                halves[h][0][p, zz, where[d1], where[d2]] = (
                    r[h * half:(h + 1) * half, dp * HD:(dp + 1) * HD])

    def keep1(p, h, zz, v2, r):
        d1, d2 = ORDER[h]
        part, r1 = halves[h][0], halves[h][1]
        total = part[p, zz, at[d1], v2, sub(p, r)].astype(jnp.float32)
        for k1 in range(1, dims[d1]):
            total += r1[p, k1 - 1, zz, v2, sub(p, r)].astype(jnp.float32)
        return total

    def sum_second(p, zz, r):
        take_pieces(p, 2 * (dims[0] - 1) * (dims[1] - 1), rest_recv.at[p, zz, r])
        for h in range(2):
            d2 = ORDER[h][1]
            sum2, r2 = halves[h][2], halves[h][3]
            for k2 in range(1, dims[d2]):
                v2 = (at[d2] + k2) % dims[d2]
                sum2[p, k2 - 1, zz, sub(p, r)] = keep1(p, h, zz, v2, r).astype(jnp.bfloat16)
                send(sum2.at[p, k2 - 1, zz, sub(p, r)], r2.at[p, k2 - 1, zz, sub(p, r)], halves[h][6].at[p],
                     second_recv.at[p, zz, r], target(dims, at, core, d2, k2)).start()

    def take_second(p, zz, r):
        take_pieces(p, dims[0] + dims[1] - 2, same_recv.at[p, zz, r])
        take_pieces(p, dims[0] + dims[1] - 2, second_recv.at[p, zz, r])

    def keep2(p, h, zz, r):
        total = keep1(p, h, zz, at[ORDER[h][1]], r)
        for k2 in range(1, dims[ORDER[h][1]]):
            total += halves[h][3][p, k2 - 1, zz, sub(p, r)].astype(jnp.float32)
        return total

    def sum_third(p, step, r):
        zz = turn(step)
        take_second(p, zz, r)
        for h in range(2):
            d1, d2 = ORDER[h]
            part, r3 = halves[h][0], halves[h][4]
            part[p, zz, at[d1], at[d2], sub(p, r)] = keep2(p, h, zz, r).astype(jnp.bfloat16)
            send(part.at[p, zz, at[d1], at[d2], sub(p, r)], r3.at[p, step - 1, sub(p, r)], halves[h][7].at[p],
                 halves[h][8].at[p], target(dims, at, core, 2, step)).start()

    def finish(p):
        size = half // cut(p)
        for r in range(cut(p)):
            take_second(p, at[2], r)
        for h in range(2):
            take_bytes(halves[h][4].at[p], halves[h][8].at[p])
            for r in range(cut(p)):
                total = keep2(p, h, at[2], r)
                for k in range(1, depth):
                    total += halves[h][4][p, k - 1, sub(p, r)].astype(jnp.float32)
                grad[h * half + r * size:h * half + (r + 1) * size, p * HD:(p + 1) * HD] = total

    def drain_reduce(p):
        for h in range(2):
            sent_bytes(halves[h][1].at[p], halves[h][5].at[p])
            sent_bytes(halves[h][3].at[p], halves[h][6].at[p])
            sent_bytes(halves[h][4].at[p], halves[h][7].at[p])


    points = [pltpu.make_async_copy(ref, pts.at[i], load_sem.at[i])
              for i, ref in enumerate((start_ref, mid_ref, end_ref))]
    wholes = [pltpu.make_async_copy(ref, dst, load_sem.at[3 + i])
              for i, (ref, dst) in enumerate(((hidden_ref, hid), (query_ref, qv), (cot_ref, gv)))]
    for load in points + wholes:
        load.start()
    barrier = pltpu.get_barrier_semaphore()
    peers = all_peers(dims, at, core)
    for peer in peers:
        pl.semaphore_signal(barrier, inc=1, device_id=peer, device_id_type=MESH)
    for load in points:
        load.wait()
    t_value = t_ref[0]
    blended = (
        (1.0 - t_value) * (1.0 - t_value) * pts[0].astype(jnp.float32)
        + 2.0 * t_value * (1.0 - t_value) * pts[1].astype(jnp.float32)
        + t_value * t_value * pts[2].astype(jnp.float32)
    ).astype(jnp.bfloat16)
    col = pl.multiple_of((at[0] * dims[1] + at[1]) * HD, HD)
    for p in range(groups):
        full[p, core, at[2], :, pl.ds(col, HD)] = blended[:, p * HD:(p + 1) * HD]
    pl.semaphore_wait(barrier, len(peers))

    def send_both(p, zz):
        for h in range(2):
            send_all(p, h, zz)

    own_z(0)
    for p in range(min(groups, 2)):
        send_both(p, at[2])

    @pl.loop(0, depth)
    def _(zz):
        swap_x(zz).start()

    cosine, sine_t = rope_tables(*cos_ref.shape)
    cos_ref[...] = cosine
    sin_ref[...] = sine_t

    def take_first_group(k):
        near(k, lambda zz, side: take_z(0, zz, side))

    def relay_first_group(k):
        near(k, lambda zz, side: relay_second(0, zz))

    take_first_group(1)
    relay_second(0, at[2])

    @pl.loop(2, depth)
    def _(k):
        take_first_group(k)
        if groups > 1:
            pl.when(k == depth - 2)(lambda: own_z(1))
        relay_first_group(k - 1)

    wholes[0].wait()
    if groups > 1:
        near(1, lambda zz, side: take_z(1, zz, side, False))
    third(0, at[2], True)
    relay_first_group(depth - 1)
    if groups > 1:
        near(1, lambda zz, side: send_both(1, zz))
    near(1, lambda zz, side: third(0, zz))
    from_core(0, at[2])

    @pl.loop(2, depth)
    def _(k):
        if groups > 1:
            pl.when(k < depth - 1)(lambda: near(k, lambda zz, side: take_z(1, zz, side)))
        near(k, lambda zz, side: third(0, zz))
        near(k - 1, lambda zz, side: from_core(0, zz))

    near(depth - 1, lambda zz, side: from_core(0, zz))
    if groups > 1:
        near(depth - 1, lambda zz, side: take_z(1, zz, side))
    wholes[1].wait()
    wholes[2].wait()

    def around(act):
        @pl.loop(0, depth)
        def _(i):
            act(turn(i))

    share = depth // heads
    early_steps = min(2, depth - 1)
    for p in range(groups):
        if p > 0:
            around(lambda zz: third(p, zz))
            around(lambda zz: from_core(p, zz))

            @pl.loop(1, early_steps + 1)
            def _(step):
                sum_second(p - 1, turn(step), 0)

            @pl.loop(1, early_steps + 1)
            def _(step):
                first_copies(p - 1, turn(step), 0, 1)
        kv[...] = acc[...].astype(jnp.bfloat16)
        if p < last:
            acc[...] = jnp.zeros_like(acc)

        @pl.loop(0, heads)
        def _(d):
            keys_at = pl.ds(pl.multiple_of(d * HD, HD), HD)
            values_at = pl.ds(pl.multiple_of((heads + d) * HD, HD), HD)
            width = qv.shape[1] // (heads * groups)
            attend_head(keys_at, values_at, ((d * groups + p) * width, width), kv, qv, gv, cos_ref,
                        sin_ref, ctx, y1.at[p], kg, vg)
            swap_y(p, keys_at)
            swap_y(p, values_at)
            if p < last:
                @pl.loop(0, share)
                def _(i):
                    k = d * share + i
                    pl.when(k == 0)(lambda: relay_second(p + 1, at[2]))
                    pl.when(k > 0)(lambda: near(k, lambda zz, side: relay_second(p + 1, zz)))
            if p > 0:
                @pl.when(d == 0)
                def _():
                    @pl.loop(early_steps + 1, depth + 1)
                    def _(step):
                        sum_second(p - 1, turn(step), 0)
                        first_copies(p - 1, turn(step), 0, 1)

        if p > 0:
            @pl.loop(1, early_steps + 1)
            def _(step):
                sum_third(p - 1, step, 0)
        partial_own(p, turn(1))
        partial_own(p, turn(2))
        if p == 0:
            take_bytes(x2, x_recv.at[0])
        take_bytes(y2.at[p], y_recv.at[p])
        if p < last:
            @pl.loop(1, depth + 1)
            def _(step):
                pl.when(step > 2)(lambda: partial_own(p, turn(step)))
                partial_sum(p, turn(step))
                first_copies(p, turn(step), 0, 0)

    def slot(n):
        i = n // 2 + 1
        return jnp.where(i == 1, 2, jnp.where(i == 2, 1, i)), n % 2

    def first_of(n, same):
        step, r = slot(n)
        first_copies(last, turn(step), r, same)

    def third_of(n):
        step, r = slot(n)
        sum_third(last, step, r)

    items = 2 * depth
    partial_sum(last, turn(2))
    for same in range(2):
        for n in range(2):
            first_of(n, same)
    partial_sum(last, turn(1))
    first_of(2, 0)

    @pl.loop(3, depth + 1)
    def _(step):
        partial_own(last, turn(step))
        partial_sum(last, turn(step))

    for p in range(last):
        @pl.loop(early_steps + 1, depth)
        def _(step):
            sum_third(p, step, 0)

    own = items - 2

    @pl.loop(0, own)
    def _(n):
        step, r = slot(n)
        sum_second(last, turn(step), r)
        pl.when(n + 2 < own)(lambda: first_of(n + 2, 1))
        pl.when(n + 3 < own)(lambda: first_of(n + 3, 0))

        for same in range(2):
            @pl.when(n == own - 2 + same)
            def _():
                first_of(own, same)
                first_of(own + 1, same)

        pl.when(n > 0)(lambda: third_of(n - 1))

    for n in (own, own + 1):
        sum_second(last, at[2], n - own)
    third_of(own - 1)
    drain_gather()
    sent_bytes(x2, x_send.at[0])
    for p in range(groups):
        sent_bytes(y1.at[p], y_send.at[p])
    for p in range(last):
        finish(p)
        drain_reduce(p)
    finish(last)
    drain_reduce(last)


def run_step(dims, hidden, queries, cotangent, point_start, point_mid, point_end, curve_time):
    rows, cols = point_mid.shape
    seq = hidden.shape[0]
    a, b, z = dims
    groups = cols // HD
    half = rows // 2
    width = a * b * HD
    sem = pltpu.SemaphoreType.DMA

    def vm(*shape, dtype=jnp.bfloat16):
        return pltpu.VMEM(shape, dtype)

    f32 = jnp.float32
    scratch = [
        vm(3, rows, cols), vm(*hidden.shape), vm(seq, z * rows),
        vm(*queries.shape), vm(*cotangent.shape),
        vm(seq, HD, dtype=f32), vm(seq, HD, dtype=f32),
        vm(groups, 2, z, rows, width), vm(seq, width, dtype=f32), vm(seq, width),
        vm(seq, HD, dtype=f32), vm(seq, HD, dtype=f32),
        vm(groups, seq, width), vm(groups, seq, width), vm(z, rows, width, dtype=f32),
        sem((6,)), sem((1,)), sem((1,)), sem((groups,)), sem((groups,)),
        sem((groups, 2, z)), sem((groups,)), sem((groups,)), sem((groups,)),
        sem((groups, 2, z)), sem((groups, 2, z)), sem((groups, z)),
        sem((groups, z, 2)), sem((groups, z, 2)), sem((groups, z, 2)),
    ]
    scratch += [sem((groups, z, dims[ORDER[1 - h][0]] - 1)) for h in range(2)]
    for h in range(2):
        n1, n2 = dims[ORDER[h][0]], dims[ORDER[h][1]]
        scratch += [
            vm(groups, z, n1, n2, half, HD), vm(groups, n1 - 1, z, n2, half, HD),
            vm(groups, n2 - 1, z, half, HD), vm(groups, n2 - 1, z, half, HD),
            vm(groups, z - 1, half, HD),
            sem((groups,)), sem((groups,)), sem((groups,)), sem((groups,)),
        ]
    hbm = pl.BlockSpec(memory_space=pl.ANY)
    return pl.pallas_call(
        functools.partial(step_kernel, dims),
        out_shape=(
            pltpu.VMEM(queries.shape, jnp.bfloat16),
            pltpu.VMEM((rows, cols), f32),
        ),
        in_specs=[pl.BlockSpec(memory_space=pltpu.SMEM)] + [hbm] * 6,
        out_specs=(pl.BlockSpec(memory_space=pltpu.VMEM),) * 2,
        scratch_shapes=scratch,
        compiler_params=pltpu.CompilerParams(
            collective_id=1, has_side_effects=True, vmem_limit_bytes=VMEM_LIMIT),
        name="bezier_step",
    )(curve_time, point_start, point_mid, point_end, hidden, queries, cotangent)


def close_kernel(t_ref, ctx_ref, grad_ref, out_ctx, out_grad, scaled, sems):
    context = pltpu.make_async_copy(ctx_ref, out_ctx, sems.at[0])
    context.start()
    t_value = t_ref[0]
    scaled[...] = grad_ref[...] * (2.0 * t_value * (1.0 - t_value))
    gradient = pltpu.make_async_copy(scaled, out_grad, sems.at[1])
    gradient.start()
    context.wait()
    gradient.wait()


def close_step(curve_time, context, gradient):
    hbm = pl.BlockSpec(memory_space=pl.ANY)
    return pl.pallas_call(
        close_kernel,
        out_shape=(
            jax.ShapeDtypeStruct(context.shape, context.dtype),
            jax.ShapeDtypeStruct(gradient.shape, gradient.dtype),
        ),
        in_specs=[pl.BlockSpec(memory_space=pltpu.SMEM), hbm, pl.BlockSpec(memory_space=pltpu.VMEM)],
        out_specs=(hbm, hbm),
        scratch_shapes=[pltpu.VMEM(gradient.shape, gradient.dtype), pltpu.SemaphoreType.DMA((2,))],
        compiler_params=pltpu.CompilerParams(vmem_limit_bytes=8 * 1024 * 1024),
        name="close_step",
    )(curve_time, context, gradient)


def local(dims, hidden, queries, cotangent, point_start, point_mid, point_end, curve_time):
    return close_step(curve_time, *run_step(
        dims, hidden, queries, cotangent, point_start, point_mid, point_end, curve_time))


def solution(mesh):
    dp, fsdp = mesh.shape["dp"], mesh.shape["fsdp"]
    dims = (dp // 2, 2, fsdp // 2)
    return jax.shard_map(
        functools.partial(local, dims),
        mesh=mesh,
        in_specs=(
            P(("dp", "fsdp"), None),
            P(("dp", "fsdp"), None),
            P(("dp", "fsdp"), None),
            P("fsdp", "dp"),
            P("fsdp", "dp"),
            P("fsdp", "dp"),
            P(),
        ),
        out_specs=(P(("dp", "fsdp"), None), P("fsdp", "dp")),
        check_vma=False,
    )
```

```python
import functools
import math

import jax
import jax.numpy as jnp
from jax import lax
from jax.experimental import pallas as pl
from jax.experimental.pallas import tpu as pltpu
from jax.sharding import PartitionSpec as P

HD = 128
BQ = 256
MESH = pl.DeviceIdType.MESH
VMEM_LIMIT = 60 * 1024 * 1024


def rope_tables(seq_len, head_dim):
    shape = (seq_len, head_dim)
    positions = lax.broadcasted_iota(jnp.int32, shape, 0).astype(jnp.float32)
    column = lax.broadcasted_iota(jnp.int32, shape, 1)
    halves_index = jnp.where(column < head_dim // 2, column, column - head_dim // 2).astype(jnp.float32)
    inverse = jnp.exp(-(2.0 * halves_index / head_dim) * math.log(500000.0))
    angles = positions * inverse
    cosine, sine_t = jnp.cos(angles), jnp.sin(angles)
    return (cosine, sine_t)


def rotate(x):
    half = x.shape[-1] // 2
    return jnp.concatenate([-x[..., half:], x[..., :half]], axis=-1)


def rotate_back(x):
    half = x.shape[-1] // 2
    return jnp.concatenate([x[..., half:], -x[..., :half]], axis=-1)


NN = (((1,), (0,)), ((), ()))
NT = (((1,), (1,)), ((), ()))
TN = (((0,), (0,)), ((), ()))


def mm(x, y, dims=NN):
    return lax.dot_general(x, y, dims, preferred_element_type=jnp.float32)


ORDER = ((1, 0), (0, 1))


def place(dims):
    dp, fs = lax.axis_index("dp"), lax.axis_index("fsdp")
    return (dp // dims[1], dp % dims[1], fs // 2), fs % 2


def target(dims, at, core, axis=None, offset=0):
    at = list(at)
    if axis is not None:
        at[axis] = (at[axis] + offset + dims[axis]) % dims[axis]
    return (at[0] * dims[1] + at[1], at[2] * 2 + core)


def send(src, dst, send_sem, recv_sem, peer):
    return pltpu.make_async_remote_copy(
        src_ref=src, dst_ref=dst, send_sem=send_sem, recv_sem=recv_sem,
        device_id=peer, device_id_type=MESH)


def all_peers(dims, at, core):
    peers = [target(dims, at, core, axis, k) for axis in range(3) for k in range(1, dims[axis])]
    return peers + [target(dims, at, 1 - core)]


def attend_head(keys_at, values_at, q_cols, kv, q_ref, g_ref, cos_ref, sin_ref, ctx_ref, y_ref, kg, vg):
    seq = kv.shape[0]
    group = q_cols[1] // HD
    scale = 1.0 / math.sqrt(HD)
    to_base2 = scale * math.log2(math.e)

    def cols(g):
        return pl.ds(pl.multiple_of(q_cols[0] + g * HD, HD), HD)

    raw = kv[:, keys_at].astype(jnp.float32)
    cosine, sine_t = cos_ref[...], sin_ref[...]
    keys = (raw * cosine + rotate(raw) * sine_t).astype(jnp.bfloat16)
    values = kv[:, values_at]
    values_t = values.astype(jnp.float32).T.astype(jnp.bfloat16)
    kg[...] = jnp.zeros_like(kg)
    vg[...] = jnp.zeros_like(vg)
    for start in range(0, seq, BQ):
        nk = start + BQ
        rows = slice(start, nk)
        qs = jnp.concatenate([q_ref[rows, cols(g)] for g in range(group)], axis=0)
        gs = jnp.concatenate([g_ref[rows, cols(g)] for g in range(group)], axis=0)
        s = mm(keys[:nk], qs, NT)
        key_at = lax.broadcasted_iota(jnp.int32, (BQ, group * BQ), 0)
        query_at = lax.broadcasted_iota(jnp.int32, (BQ, group * BQ), 1) % BQ
        last = jnp.where(key_at <= query_at, s[start:], -1e30)
        s = last if start == 0 else jnp.concatenate([s[:start], last], axis=0)
        top = jnp.max(s, axis=0, keepdims=True)
        w = jnp.exp2((s - top) * to_base2)
        p = w * (1.0 / jnp.sum(w, axis=0, keepdims=True))
        p_low = p.astype(jnp.bfloat16)
        ctx_t = mm(values_t[:, :nk], p_low)
        dp = mm(values[:nk], gs, NT)
        vg[:nk] += mm(p_low, gs)
        delta = jnp.sum(dp * p, axis=0, keepdims=True)
        ds = (p * ((dp - delta) * scale)).astype(jnp.bfloat16)
        kg[:nk] += mm(ds, qs)
        ctx = ctx_t.T.astype(jnp.bfloat16)
        for g in range(group):
            ctx_ref[rows, cols(g)] = ctx[g * BQ:(g + 1) * BQ]
    rot = kg[...]
    y_ref[:, keys_at] = (rot * cosine + rotate_back(rot * sine_t)).astype(jnp.bfloat16)
    y_ref[:, values_at] = vg[...].astype(jnp.bfloat16)


def step_kernel(dims, t_ref, start_ref, mid_ref, end_ref, hidden_ref, query_ref, cot_ref, ctx, grad,
                pts, hid, x2, qv, gv, cos_ref, sin_ref, full, acc, kv, kg, vg, y1, y2, early,
                load_sem, x_send, x_recv, y_send, y_recv, z_send, s_send, t_send, c_send,
                z_recv, t_recv, c_recv, same_recv, rest_recv, second_recv, *more):
    s_recv = more[:2]
    halves = [more[2:11], more[11:20]]
    at, core = place(dims)
    depth = dims[2]
    across = dims[0] * dims[1]
    rows = start_ref.shape[0]
    half = rows // 2
    groups = full.shape[0]
    last = groups - 1
    heads = across // 2
    other = target(dims, at, 1 - core)
    here = at[:2]

    def take_bytes(ref, sem):
        send(ref, ref, c_send.at[0], sem, other).wait_recv()

    def sent_bytes(ref, sem):
        send(ref, ref, sem, c_recv.at[0, 0], other).wait_send()


    def piece(p, c, h, zz, pos):
        col = pl.multiple_of((pos[0] * dims[1] + pos[1]) * HD, HD)
        return full.at[p, c, zz, pl.ds(h * half, half), pl.ds(col, HD)]

    def moved(axis, k):
        pos = [at[0], at[1]]
        pos[axis] = (pos[axis] + k) % dims[axis]
        return pos

    def push(p, h, zz, pos, send_sem, recv_sem, peer):
        ref = piece(p, core, h, zz, pos)
        return send(ref, ref, send_sem, recv_sem, peer)

    def near(k, act):
        @pl.loop(0, 2)
        def _(side):
            zz = at[2] + (2 * side - 1) * k
            pl.when((zz >= 0) & (zz < depth))(lambda: act(zz, side))

    def to_z(p, h, zz, side):
        push(p, h, zz, here, z_send.at[p, zz + side], z_recv.at[p, h, zz],
             target(dims, at, core, 2, 1 - 2 * side)).start()

    def onward(side):
        return ((side == 0) & (at[2] < depth - 1)) | ((side == 1) & (at[2] > 0))

    def to_second(p, h, zz, k):
        push(p, h, zz, here, s_send.at[p], s_recv[h].at[p, zz, k - 1],
             target(dims, at, core, ORDER[1 - h][0], k)).start()

    def to_third(p, h, zz, pos, k):
        push(p, h, zz, pos, t_send.at[p], t_recv.at[p, zz],
             target(dims, at, core, ORDER[1 - h][1], k)).start()

    def to_core(p, h, zz, pos):
        push(p, h, zz, pos, c_send.at[p], c_recv.at[p, zz], other).start()

    def swap_x(zz):
        src = pl.multiple_of((2 * zz + 1 - core) * rows, rows)
        dst = pl.multiple_of(zz * rows, rows)
        return send(hidden_ref.at[:, pl.ds(src, rows)], x2.at[:, pl.ds(dst, rows)],
                    x_send.at[0], x_recv.at[0], other)

    def own_z(p):
        @pl.loop(0, 2)
        def _(side):
            @pl.when(onward(side))
            def _():
                for h in range(2):
                    to_z(p, h, at[2], side)

    def send_all(p, h, zz):
        for k in range(1, dims[ORDER[1 - h][0]]):
            to_second(p, h, zz, k)
        for k in range(1, dims[ORDER[1 - h][1]]):
            to_third(p, h, zz, here, k)
        to_core(p, h, zz, here)

    def take_z(p, zz, side, more=True):
        for h in range(2):
            take_bytes(piece(p, core, h, zz, here), z_recv.at[p, h, zz])
            pl.when(onward(side))(lambda: to_z(p, h, zz, side))
            if more:
                send_all(p, h, zz)

    def relay_second(p, zz):
        for h in range(2):
            d2, d3 = ORDER[1 - h]
            for k2 in range(1, dims[d2]):
                pos = moved(d2, k2)
                take_bytes(piece(p, core, h, zz, pos), s_recv[h].at[p, zz, dims[d2] - k2 - 1])
                for k in range(1, dims[d3]):
                    to_third(p, h, zz, pos, k)
                to_core(p, h, zz, pos)

    def product(p, c, zz, first=False):
        x = hid[:, pl.ds(pl.multiple_of((2 * zz + c) * rows, rows), rows)]
        got = mm(x, full[p, c, zz])
        if first:
            acc[...] = got
        else:
            acc[...] += got

    def third(p, zz, first=False):
        count = (2 * across - dims[0] - dims[1]) // 2
        take_bytes(full.at[p, core, zz, :, pl.ds(0, count * HD)], t_recv.at[p, zz])
        for h in range(2):
            d2, d3 = ORDER[1 - h]
            for k3 in range(1, dims[d3]):
                for k2 in range(dims[d2]):
                    pos = moved(d3, k3)
                    pos[d2] = (at[d2] + k2) % dims[d2]
                    to_core(p, h, zz, pos)
        product(p, core, zz, first)

    def from_core(p, zz):
        take_bytes(full.at[p, 1 - core, zz], c_recv.at[p, zz])
        product(p, 1 - core, zz)

    def drain_gather():
        seconds = dims[0] + dims[1] - 2
        thirds = (2 * across - dims[0] - dims[1]) // 2
        for p in range(groups):
            @pl.loop(0, depth)
            def _(zz):
                ref = full.at[p, core, zz, :, pl.ds(0, HD)]
                pl.when((zz <= at[2]) & (at[2] < depth - 1))(lambda: sent_bytes(ref, z_send.at[p, zz]))
                pl.when((zz >= at[2]) & (at[2] > 0))(lambda: sent_bytes(ref, z_send.at[p, zz + 1]))

            sent_bytes(full.at[p, core, :, pl.ds(0, half), pl.ds(0, seconds * HD)], s_send.at[p])
            sent_bytes(full.at[p, core, :, :, pl.ds(0, thirds * HD)], t_send.at[p])
            sent_bytes(full.at[p, core], c_send.at[p])


    def cut(p):
        return 2 if p == last else 1

    def sub(p, r):
        size = half // cut(p)
        return pl.ds(pl.multiple_of(r * size, size), size)

    def take_pieces(p, count, sem):
        take_bytes(full.at[0, core, 0, pl.ds(0, half // cut(p)), pl.ds(0, count * HD)], sem)

    def first_copies(p, zz, r, same):
        for h in range(2):
            d1, d2 = ORDER[h]
            part, r1 = halves[h][0], halves[h][1]
            sem = (same_recv if same else rest_recv).at[zz, p + r]
            for k1 in range(1, dims[d1]):
                v1 = (at[d1] + k1) % dims[d1]
                for k2 in (0,) if same else range(1, dims[d2]):
                    v2 = (at[d2] + k2) % dims[d2]
                    send(part.at[p, zz, v1, v2, sub(p, r)], r1.at[p, k1 - 1, zz, v2, sub(p, r)],
                         halves[h][5].at[p], sem, target(dims, at, core, d1, k1)).start()

    def swap_y(p, columns):
        send(y1.at[p, :, columns], y2.at[p, :, columns], y_send.at[p], y_recv.at[p], other).start()

    def partial_own(p, zz):
        x = hid[:, pl.ds(pl.multiple_of((2 * zz + core) * rows, rows), rows)]
        early[zz] = mm(x, y1[p], TN)

    def turn(step):
        return (at[2] + step) % depth

    def partial_sum(p, zz):
        x = x2[:, pl.ds(pl.multiple_of(zz * rows, rows), rows)]
        r = (early[zz] + mm(x, y2[p], TN)).astype(jnp.bfloat16)
        for dp in range(across):
            where = (dp // dims[1], dp % dims[1])
            for h in range(2):
                d1, d2 = ORDER[h]
                halves[h][0][p, zz, where[d1], where[d2]] = (
                    r[h * half:(h + 1) * half, dp * HD:(dp + 1) * HD])

    def keep1(p, h, zz, v2, r):
        d1, d2 = ORDER[h]
        part, r1 = halves[h][0], halves[h][1]
        total = part[p, zz, at[d1], v2, sub(p, r)].astype(jnp.float32)
        for k1 in range(1, dims[d1]):
            total += r1[p, k1 - 1, zz, v2, sub(p, r)].astype(jnp.float32)
        return total

    def sum_second(p, zz, r):
        take_pieces(p, 2 * (dims[0] - 1) * (dims[1] - 1), rest_recv.at[zz, p + r])
        for h in range(2):
            d2 = ORDER[h][1]
            sum2, r2 = halves[h][2], halves[h][3]
            for k2 in range(1, dims[d2]):
                v2 = (at[d2] + k2) % dims[d2]
                sum2[p, k2 - 1, zz, sub(p, r)] = keep1(p, h, zz, v2, r).astype(jnp.bfloat16)
                send(sum2.at[p, k2 - 1, zz, sub(p, r)], r2.at[p, k2 - 1, zz, sub(p, r)], halves[h][6].at[p],
                     second_recv.at[zz, p + r], target(dims, at, core, d2, k2)).start()

    def take_second(p, zz, r):
        take_pieces(p, dims[0] + dims[1] - 2, same_recv.at[zz, p + r])
        take_pieces(p, dims[0] + dims[1] - 2, second_recv.at[zz, p + r])

    def keep2(p, h, zz, r):
        total = keep1(p, h, zz, at[ORDER[h][1]], r)
        for k2 in range(1, dims[ORDER[h][1]]):
            total += halves[h][3][p, k2 - 1, zz, sub(p, r)].astype(jnp.float32)
        return total

    def sum_third(p, step, r):
        zz = turn(step)
        take_second(p, zz, r)
        for h in range(2):
            d1, d2 = ORDER[h]
            part, r3 = halves[h][0], halves[h][4]
            part[p, zz, at[d1], at[d2], sub(p, r)] = keep2(p, h, zz, r).astype(jnp.bfloat16)
            send(part.at[p, zz, at[d1], at[d2], sub(p, r)], r3.at[p, step - 1, sub(p, r)], halves[h][7].at[p],
                 halves[h][8].at[p], target(dims, at, core, 2, step)).start()

    def finish(p):
        size = half // cut(p)
        for r in range(cut(p)):
            take_second(p, at[2], r)
        for h in range(2):
            take_bytes(halves[h][4].at[p], halves[h][8].at[p])
            for r in range(cut(p)):
                total = keep2(p, h, at[2], r)
                for k in range(1, depth):
                    total += halves[h][4][p, k - 1, sub(p, r)].astype(jnp.float32)
                grad[h * half + r * size:h * half + (r + 1) * size, p * HD:(p + 1) * HD] = total

    def drain_reduce(p):
        for h in range(2):
            sent_bytes(halves[h][1].at[p], halves[h][5].at[p])
            sent_bytes(halves[h][3].at[p], halves[h][6].at[p])
            sent_bytes(halves[h][4].at[p], halves[h][7].at[p])


    points = [pltpu.make_async_copy(ref, pts.at[i], load_sem.at[i])
              for i, ref in enumerate((start_ref, mid_ref, end_ref))]
    wholes = [pltpu.make_async_copy(ref, dst, load_sem.at[3 + i])
              for i, (ref, dst) in enumerate(((hidden_ref, hid), (query_ref, qv), (cot_ref, gv)))]
    for load in points + wholes:
        load.start()
    barrier = pltpu.get_barrier_semaphore()
    peers = all_peers(dims, at, core)
    for peer in peers:
        pl.semaphore_signal(barrier, inc=1, device_id=peer, device_id_type=MESH)
    for load in points:
        load.wait()
    t_value = t_ref[0]
    blended = (
        (1.0 - t_value) * (1.0 - t_value) * pts[0].astype(jnp.float32)
        + 2.0 * t_value * (1.0 - t_value) * pts[1].astype(jnp.float32)
        + t_value * t_value * pts[2].astype(jnp.float32)
    ).astype(jnp.bfloat16)
    col = pl.multiple_of((at[0] * dims[1] + at[1]) * HD, HD)
    for p in range(groups):
        full[p, core, at[2], :, pl.ds(col, HD)] = blended[:, p * HD:(p + 1) * HD]
    pl.semaphore_wait(barrier, len(peers))

    def send_both(p, zz):
        for h in range(2):
            send_all(p, h, zz)

    own_z(0)
    for p in range(min(groups, 2)):
        send_both(p, at[2])

    @pl.loop(0, depth)
    def _(zz):
        swap_x(zz).start()

    cosine, sine_t = rope_tables(*cos_ref.shape)
    cos_ref[...] = cosine
    sin_ref[...] = sine_t

    def take_first_group(k):
        near(k, lambda zz, side: take_z(0, zz, side))

    def relay_first_group(k):
        near(k, lambda zz, side: relay_second(0, zz))

    take_first_group(1)
    relay_second(0, at[2])

    @pl.loop(2, depth)
    def _(k):
        take_first_group(k)
        if groups > 1:
            pl.when(k == depth - 2)(lambda: own_z(1))
        relay_first_group(k - 1)

    wholes[0].wait()
    if groups > 1:
        near(1, lambda zz, side: take_z(1, zz, side, False))
    third(0, at[2], True)
    relay_first_group(depth - 1)
    if groups > 1:
        near(1, lambda zz, side: send_both(1, zz))
    near(1, lambda zz, side: third(0, zz))
    from_core(0, at[2])

    @pl.loop(2, depth)
    def _(k):
        if groups > 1:
            pl.when(k < depth - 1)(lambda: near(k, lambda zz, side: take_z(1, zz, side)))
        near(k, lambda zz, side: third(0, zz))
        near(k - 1, lambda zz, side: from_core(0, zz))

    near(depth - 1, lambda zz, side: from_core(0, zz))
    if groups > 1:
        near(depth - 1, lambda zz, side: take_z(1, zz, side))
    wholes[1].wait()
    wholes[2].wait()

    def around(act):
        @pl.loop(0, depth)
        def _(i):
            act(turn(i))

    share = depth // heads
    early_steps = min(2, depth - 1)
    for p in range(groups):
        if p > 0:
            around(lambda zz: third(p, zz))
            around(lambda zz: from_core(p, zz))

            @pl.loop(1, early_steps + 1)
            def _(step):
                sum_second(p - 1, turn(step), 0)

            @pl.loop(1, early_steps + 1)
            def _(step):
                first_copies(p - 1, turn(step), 0, 1)
        kv[...] = acc[...].astype(jnp.bfloat16)
        if p < last:
            acc[...] = jnp.zeros_like(acc)

        @pl.loop(0, heads)
        def _(d):
            keys_at = pl.ds(pl.multiple_of(d * HD, HD), HD)
            values_at = pl.ds(pl.multiple_of((heads + d) * HD, HD), HD)
            width = qv.shape[1] // (heads * groups)
            attend_head(keys_at, values_at, ((d * groups + p) * width, width), kv, qv, gv, cos_ref,
                        sin_ref, ctx, y1.at[p], kg, vg)
            swap_y(p, keys_at)
            swap_y(p, values_at)
            if p < last:
                @pl.loop(0, share)
                def _(i):
                    k = d * share + i
                    pl.when(k == 0)(lambda: relay_second(p + 1, at[2]))
                    pl.when(k > 0)(lambda: near(k, lambda zz, side: relay_second(p + 1, zz)))
            if p > 0:
                @pl.when(d == 0)
                def _():
                    @pl.loop(early_steps + 1, depth + 1)
                    def _(step):
                        sum_second(p - 1, turn(step), 0)
                        first_copies(p - 1, turn(step), 0, 1)

        if p > 0:
            @pl.loop(1, early_steps + 1)
            def _(step):
                sum_third(p - 1, step, 0)
        partial_own(p, turn(1))
        partial_own(p, turn(2))
        if p == 0:
            take_bytes(x2, x_recv.at[0])
        take_bytes(y2.at[p], y_recv.at[p])
        if p < last:
            @pl.loop(1, depth + 1)
            def _(step):
                pl.when(step > 2)(lambda: partial_own(p, turn(step)))
                partial_sum(p, turn(step))
                first_copies(p, turn(step), 0, 0)

    def slot(n):
        i = n // 2 + 1
        return jnp.where(i == 1, 2, jnp.where(i == 2, 1, i)), n % 2

    def first_of(n, same):
        step, r = slot(n)
        first_copies(last, turn(step), r, same)

    def third_of(n):
        step, r = slot(n)
        sum_third(last, step, r)

    items = 2 * depth
    partial_sum(last, turn(2))
    for same in range(2):
        for n in range(2):
            first_of(n, same)
    partial_sum(last, turn(1))
    first_of(2, 0)

    @pl.loop(3, depth + 1)
    def _(step):
        partial_own(last, turn(step))
        partial_sum(last, turn(step))

    for p in range(last):
        @pl.loop(early_steps + 1, depth)
        def _(step):
            sum_third(p, step, 0)

    own = items - 2

    @pl.loop(0, own)
    def _(n):
        step, r = slot(n)
        sum_second(last, turn(step), r)
        pl.when(n + 2 < own)(lambda: first_of(n + 2, 1))
        pl.when(n + 3 < own)(lambda: first_of(n + 3, 0))

        for same in range(2):
            @pl.when(n == own - 2 + same)
            def _():
                first_of(own, same)
                first_of(own + 1, same)

        pl.when(n > 0)(lambda: third_of(n - 1))

    for n in (own, own + 1):
        sum_second(last, at[2], n - own)
    third_of(own - 1)
    drain_gather()
    sent_bytes(x2, x_send.at[0])
    for p in range(groups):
        sent_bytes(y1.at[p], y_send.at[p])
    for p in range(last):
        finish(p)
        drain_reduce(p)
    finish(last)
    drain_reduce(last)


def run_step(dims, hidden, queries, cotangent, point_start, point_mid, point_end, curve_time):
    rows, cols = point_mid.shape
    seq = hidden.shape[0]
    a, b, z = dims
    groups = cols // HD
    half = rows // 2
    width = a * b * HD
    sem = pltpu.SemaphoreType.DMA

    def vm(*shape, dtype=jnp.bfloat16):
        return pltpu.VMEM(shape, dtype)

    f32 = jnp.float32
    scratch = [
        vm(3, rows, cols), vm(*hidden.shape), vm(seq, z * rows),
        vm(*queries.shape), vm(*cotangent.shape),
        vm(seq, HD, dtype=f32), vm(seq, HD, dtype=f32),
        vm(groups, 2, z, rows, width), vm(seq, width, dtype=f32), vm(seq, width),
        vm(seq, HD, dtype=f32), vm(seq, HD, dtype=f32),
        vm(groups, seq, width), vm(groups, seq, width), vm(z, rows, width, dtype=f32),
        sem((6,)), sem((1,)), sem((1,)), sem((groups,)), sem((groups,)),
        sem((groups, z + 1)), sem((groups,)), sem((groups,)), sem((groups,)),
        sem((groups, 2, z)), sem((groups, z)), sem((groups, z)),
        sem((z, groups + 1)), sem((z, groups + 1)), sem((z, groups + 1)),
    ]
    scratch += [sem((groups, z, dims[ORDER[1 - h][0]] - 1)) for h in range(2)]
    for h in range(2):
        n1, n2 = dims[ORDER[h][0]], dims[ORDER[h][1]]
        scratch += [
            vm(groups, z, n1, n2, half, HD), vm(groups, n1 - 1, z, n2, half, HD),
            vm(groups, n2 - 1, z, half, HD), vm(groups, n2 - 1, z, half, HD),
            vm(groups, z - 1, half, HD),
            sem((groups,)), sem((groups,)), sem((groups,)), sem((groups,)),
        ]
    hbm = pl.BlockSpec(memory_space=pl.ANY)
    return pl.pallas_call(
        functools.partial(step_kernel, dims),
        out_shape=(
            pltpu.VMEM(queries.shape, jnp.bfloat16),
            pltpu.VMEM((rows, cols), f32),
        ),
        in_specs=[pl.BlockSpec(memory_space=pltpu.SMEM)] + [hbm] * 6,
        out_specs=(pl.BlockSpec(memory_space=pltpu.VMEM),) * 2,
        scratch_shapes=scratch,
        compiler_params=pltpu.CompilerParams(
            collective_id=1, has_side_effects=True, vmem_limit_bytes=VMEM_LIMIT),
        name="bezier_step",
    )(curve_time, point_start, point_mid, point_end, hidden, queries, cotangent)


def close_kernel(t_ref, ctx_ref, grad_ref, out_ctx, out_grad, scaled, sems):
    context = pltpu.make_async_copy(ctx_ref, out_ctx, sems.at[0])
    context.start()
    t_value = t_ref[0]
    scaled[...] = grad_ref[...] * (2.0 * t_value * (1.0 - t_value))
    gradient = pltpu.make_async_copy(scaled, out_grad, sems.at[1])
    gradient.start()
    context.wait()
    gradient.wait()


def close_step(curve_time, context, gradient):
    hbm = pl.BlockSpec(memory_space=pl.ANY)
    return pl.pallas_call(
        close_kernel,
        out_shape=(
            jax.ShapeDtypeStruct(context.shape, context.dtype),
            jax.ShapeDtypeStruct(gradient.shape, gradient.dtype),
        ),
        in_specs=[pl.BlockSpec(memory_space=pltpu.SMEM), hbm, pl.BlockSpec(memory_space=pltpu.VMEM)],
        out_specs=(hbm, hbm),
        scratch_shapes=[pltpu.VMEM(gradient.shape, gradient.dtype), pltpu.SemaphoreType.DMA((2,))],
        compiler_params=pltpu.CompilerParams(vmem_limit_bytes=8 * 1024 * 1024),
        name="close_step",
    )(curve_time, context, gradient)


def local(dims, hidden, queries, cotangent, point_start, point_mid, point_end, curve_time):
    return close_step(curve_time, *run_step(
        dims, hidden, queries, cotangent, point_start, point_mid, point_end, curve_time))


def solution(mesh):
    dp, fsdp = mesh.shape["dp"], mesh.shape["fsdp"]
    dims = (dp // 2, 2, fsdp // 2)
    return jax.shard_map(
        functools.partial(local, dims),
        mesh=mesh,
        in_specs=(
            P(("dp", "fsdp"), None),
            P(("dp", "fsdp"), None),
            P(("dp", "fsdp"), None),
            P("fsdp", "dp"),
            P("fsdp", "dp"),
            P("fsdp", "dp"),
            P(),
        ),
        out_specs=(P(("dp", "fsdp"), None), P("fsdp", "dp")),
        check_vma=False,
    )
```
